32 devices in a mesh: py: 4 (over y, x), pz: 8 (over z, core).
Axes of the slice: x: 2, y: 2, z: 4, core: 2. Of those that a mesh axis runs over, the one named last changes fastest.
Arguments:
- positions: float32 [3, 131072], P(None, ('py', 'pz')), may hold values from 0 to 512, as said below
- masses: float32 [131072], P(('py', 'pz')), may hold values from 16 to 160
Outputs:
- forces: float32 [3, 32, 64, 512], P(None, 'py', 'pz')
The draws below stay inside these ranges and needn't reach their ends.
Inputs may be any that keep to these rules, and one draw needn't show every extreme that they name: `positions`: the particles come in blocks of 4096 columns; in the block numbered a 8 + b, row 0 lies in [a 8, (a + 1) * 8), row 1 in [b * 8, (b + 1) * 8), and row 2 in [0, 512).
All inputs are finite; a program needn't handle non-finite values.
Results may differ from the reference program's by a relative error of at most 0.0003.
Values sent between devices are 32-bit elements; how exact they have to be, the bound alone decides.
A program may use at most 64 MiB of HBM per device.

```python
import math
import jax
import jax.numpy as jnp

NX = 512
CY = 8
CZ = 8
PART_DEV = 4096
NY = 32
NZ = 64
NPART = 131072
N_PY = 4
N_PZ = 8


def draw_positions(key, part):
    total = PART_DEV * N_PY * N_PZ
    keys = jax.random.split(jax.random.fold_in(key, 17), 3)
    owner = jnp.arange(total, dtype=jnp.int32) // PART_DEV
    block_y = (owner // N_PZ).astype(jnp.float32)
    block_z = (owner % N_PZ).astype(jnp.float32)
    along_y = jax.random.uniform(keys[0], (total,), jnp.float32)
    along_z = jax.random.uniform(keys[1], (total,), jnp.float32)
    along_x = jax.random.uniform(keys[2], (total,), jnp.float32)
    coord_y = (block_y + along_y * 0.999) * CY
    coord_z = (block_z + along_z * 0.999) * CZ
    coord_x = along_x * (NX * 0.9999)
    return jnp.stack([coord_y, coord_z, coord_x]).astype(jnp.float32)


def level_of(key, extent, pieces, low, largest):
    gain = 1.0
    for position, parts in pieces:
        heights = jax.random.uniform(jax.random.fold_in(jax.random.fold_in(key, 6), position), (parts,), jnp.float32, low / len(pieces), largest / len(pieces))
        gain = gain * jnp.repeat(jnp.exp(heights), extent[position] // parts).reshape((-1,) + (1,) * (len(extent) - 1 - position))
    return gain


def setup_inputs(seed: int = 0) -> dict:
    key_list = jax.random.split(jax.random.key(seed), 3)
    return {
        "positions": draw_positions(jax.random.fold_in(key_list[2], 71), 0),
        "masses": jnp.clip(jnp.exp(math.log(160.0) - 2.3025851 * jax.random.uniform(key_list[1], (NPART,), jnp.float32) ** level_of(key_list[1], (NPART,), ((0, 32),), -0.2, 0.2)), 16.0, 160.0),
    }


smoothing_sq = 0.25


def wave_square(count, period):
    waves = jnp.arange(count, dtype=jnp.int32)
    folded = jnp.minimum(waves, period - waves).astype(jnp.float32)
    return (folded * (2.0 * math.pi / period)) ** 2


def reference(positions, masses):
    floors = jnp.floor(positions)
    fraction = positions - floors
    corner = floors.astype(jnp.int32)
    density = jnp.zeros((NY * NZ * NX,), jnp.float32)
    for offset_y in (0, 1):
        for offset_z in (0, 1):
            for offset_x in (0, 1):
                cell_y = (corner[0] + offset_y) % NY
                cell_z = (corner[1] + offset_z) % NZ
                cell_x = (corner[2] + offset_x) % NX
                weight_y = fraction[0] if offset_y else 1.0 - fraction[0]
                weight_z = fraction[1] if offset_z else 1.0 - fraction[1]
                weight_x = fraction[2] if offset_x else 1.0 - fraction[2]
                flat_index = (cell_y * NZ + cell_z) * NX + cell_x
                density = density.at[flat_index].add(masses * weight_y * weight_z * weight_x)
    density = density.reshape(NY, NZ, NX)
    total = wave_square(NY, NY)[:, None, None] + wave_square(NZ, NZ)[None, :, None] + wave_square(NX // 2 + 1, NX)[None, None, :]
    safe_total = jnp.where(total > 0, total, 1.0)
    green = jnp.where(total > 0, -4.0 * math.pi * jnp.exp(-smoothing_sq * total) / safe_total, 0.0)
    keep_x = jnp.arange(NX // 2 + 1, dtype=jnp.int32) < NX // 2
    green = jnp.where(keep_x[None, None, :], green, 0.0)
    spectrum = jnp.fft.rfftn(density)
    potential = jnp.fft.irfftn(spectrum * green, s=(NY, NZ, NX)).astype(jnp.float32)
    force_y = (jnp.roll(potential, 1, 0) - jnp.roll(potential, -1, 0)) * 0.5
    force_z = (jnp.roll(potential, 1, 1) - jnp.roll(potential, -1, 1)) * 0.5
    force_x = (jnp.roll(potential, 1, 2) - jnp.roll(potential, -1, 2)) * 0.5
    return jnp.stack([force_y, force_z, force_x])
```

```python
import functools
import math

import jax
import jax.numpy as jnp
import ml_dtypes
import numpy as np
from jax import lax
from jax.experimental import pallas as pl
from jax.experimental.pallas import tpu as pltpu
from jax.sharding import PartitionSpec as P

MESH = pl.DeviceIdType.MESH
F32 = jnp.float32
BF16 = jnp.bfloat16
SMOOTHING_SQ = 0.25
CELL = 8
PAIR = 2 * CELL
GROUPS = 128 // PAIR


def parts(table, count):
    out = []
    for _ in range(count):
        out.append(table.astype(ml_dtypes.bfloat16))
        table = table - out[-1].astype(np.float64)
    return np.stack(out)


def tables(n_py, n_pz, nx, nf):
    ny, nz = CELL * n_py, CELL * n_pz
    kept = nx // 2
    phase = (np.outer(np.arange(kept), np.arange(nx)) % nx) * (2 * np.pi / nx)
    line = np.concatenate([np.cos(phase), -np.sin(phase)])
    phase = (np.outer(np.arange(ny), np.arange(ny)) % ny) * (2 * np.pi / ny)
    eye = np.eye(nf)
    rows = np.concatenate([np.kron(np.cos(phase), eye), np.kron(np.sin(phase), eye)], axis=1)
    phase = (np.outer(np.arange(nz), np.arange(nz)) % nz) * (2 * np.pi / nz)
    cos, sin = np.cos(phase), np.sin(phase)
    forward = np.zeros((n_pz, 2, CELL, 2, nz))
    forward[:, 0, :, 0] = cos.reshape(n_pz, CELL, nz)
    forward[:, 0, :, 1] = -sin.reshape(n_pz, CELL, nz)
    forward[:, 1, :, 0] = sin.reshape(n_pz, CELL, nz)
    forward[:, 1, :, 1] = cos.reshape(n_pz, CELL, nz)
    forward = forward.reshape(2 * nz, 2, nz)
    turned = np.stack([forward[:, 1], -forward[:, 0]], axis=1)
    forward = np.concatenate([forward.reshape(2 * nz, 2 * nz), turned.reshape(2 * nz, 2 * nz)], 1)
    inverse = np.zeros((2, nz, n_pz, 2, CELL))
    inverse[0, :, :, 0] = cos.reshape(nz, n_pz, CELL)
    inverse[0, :, :, 1] = sin.reshape(nz, n_pz, CELL)
    inverse[1, :, :, 0] = -sin.reshape(nz, n_pz, CELL)
    inverse[1, :, :, 1] = cos.reshape(nz, n_pz, CELL)
    inverse = inverse.reshape(2 * nz, n_pz, 2, CELL)
    turned = np.stack([-inverse[:, :, 1], inverse[:, :, 0]], axis=2)
    inverse = np.concatenate([inverse.reshape(2 * nz, 2 * nz), turned.reshape(2 * nz, 2 * nz)], 1)
    return parts(line, 3), parts(rows, 3), parts(forward, 2), parts(inverse, 3)


def split(x, count=2):
    out = []
    for i in range(count):
        out.append(x.astype(BF16))
        if i < count - 1:
            x = x - out[-1].astype(F32)
    return out


def dot_parts(left, right, dims=((1,), (0,))):
    count = len(left)
    total = None
    for order in reversed(range(count)):
        for i in range(order + 1):
            term = lax.dot_general(
                left[i], right[order - i], (dims, ((), ())), preferred_element_type=F32
            )
            total = term if total is None else total + term
    return total


def swap_groups(tiles):
    group = lax.broadcasted_iota(jnp.int32, tiles[0].shape, 1) // PAIR
    moved = []
    for step in range(GROUPS):
        mixed = tiles[step]
        for a in range(1, GROUPS):
            mixed = jnp.where(group == a, tiles[(a + step) % GROUPS], mixed)
        moved.append(pltpu.roll(mixed, step * PAIR, 1) if step else mixed)
    out = []
    for a in range(GROUPS):
        mixed = moved[(0 - a) % GROUPS]
        for g in range(1, GROUPS):
            mixed = jnp.where(group == g, moved[(g - a) % GROUPS], mixed)
        out.append(mixed)
    return out


def green_factor(rank, n_py, n_pz, nx, nf):
    ny, nz = CELL * n_py, CELL * n_pz
    shape = (ny * nf, 2 * nz)
    row = lax.broadcasted_iota(jnp.int32, shape, 0)
    col = lax.broadcasted_iota(jnp.int32, shape, 1)

    def square(wave, period):
        folded = jnp.minimum(wave, period - wave).astype(F32)
        return (folded * (2.0 * math.pi / period)) ** 2

    wave_x = rank * nf + row % nf
    total = square(row // nf, ny) + square(col % nz, nz) + square(wave_x, nx)
    safe = jnp.where(total > 0, total, 1.0)
    green = jnp.where(total > 0, -4.0 * math.pi * jnp.exp(-SMOOTHING_SQ * total) / safe, 0.0)
    return green * (jnp.where(wave_x > 0, 2.0, 1.0) * (1.0 / float(ny * nz * nx)))


def kernel(
    n_py, n_pz, nx, nf, chunk,
    pos_hbm, mass_hbm, line_hbm, rows_hbm, fwd_hbm, inv_hbm,
    pot_ref, side_ref,
    pos_ref, mass_ref, line, rows, fwd, inv, table_sem,
    hot, acc_halo, acc, halo_out, halo_in, halo_send, halo_recv,
    send1, recv1, field, send2, recv2, waves,
    send_sem1, recv_sem1, send_sem2, recv_sem2,
    edge_out, edge_in, edge_send, edge_recv,
):
    n = n_py * n_pz
    my_y, my_z = lax.axis_index("py"), lax.axis_index("pz")
    rank = my_y * n_pz + my_z

    loads = [
        pltpu.make_async_copy(src, dst, table_sem.at[i])
        for i, (src, dst) in enumerate(
            [
                (pos_hbm, pos_ref),
                (mass_hbm, mass_ref),
                (line_hbm, line),
                (rows_hbm, rows),
                (fwd_hbm, fwd),
                (inv_hbm, inv),
            ]
        )
    ]
    for load in loads:
        load.start()

    def coords(step):
        other_y = lax.rem(n - step, n_py) ^ my_y
        other_z = ((n - step) // n_py) ^ my_z
        return other_y * n_pz + other_z, (other_y, other_z)

    barrier = pltpu.get_barrier_semaphore()

    @pl.loop(1, n)
    def _(step):
        pl.semaphore_signal(barrier, inc=1, device_id=coords(step)[1], device_id_type=MESH)

    base_y = (my_y * CELL).astype(F32)
    base_z = (my_z * CELL).astype(F32)
    acc[...] = jnp.zeros_like(acc)
    acc_halo[...] = jnp.zeros_like(acc_halo)
    cell = lax.broadcasted_iota(jnp.int32, (CELL, chunk), 0).astype(F32)
    x_index = lax.broadcasted_iota(jnp.int32, (nx, chunk), 0).astype(F32)

    for load in loads[:2]:
        load.wait()

    def weights(turn):
        span = pl.ds(pl.multiple_of(turn * chunk, chunk), chunk)
        along_y = pos_ref[0:1, span] - base_y
        along_z = pos_ref[1:2, span] - base_z
        along_x = pos_ref[2:3, span]
        mass = mass_ref[0:1, span]
        floor_x = jnp.floor(along_x)
        frac_x = along_x - floor_x
        hat_y = jnp.maximum(1.0 - jnp.abs(along_y - cell), 0.0)
        hat_z = jnp.maximum(1.0 - jnp.abs(along_z - cell), 0.0)
        last_y = jnp.maximum(along_y - (CELL - 1.0), 0.0)
        last_z = jnp.maximum(along_z - (CELL - 1.0), 0.0)
        shares = (mass * (1.0 - frac_x), mass * frac_x)
        return span, floor_x, hat_y, hat_z, last_y, last_z, shares

    def deposited(tile_sets, one_hot):
        pairs = [split(jnp.concatenate(tiles, axis=0)) for tiles in tile_sets]
        stacked = jnp.concatenate([pair[i] for i in range(2) for pair in pairs], axis=0)
        return lax.dot_general(
            stacked, one_hot, (((1,), (1,)), ((), ())), preferred_element_type=F32
        )

    def settled(sums):
        plane = sums.shape[0] // 4
        lower = sums[0:plane] + sums[2 * plane : 3 * plane]
        upper = sums[plane : 2 * plane] + sums[3 * plane : 4 * plane]
        return lower + pltpu.roll(upper, 1, 1)

    turns = pos_ref.shape[1] // chunk

    @pl.loop(0, turns)
    def _(turn):
        span, floor_x, hat_y, hat_z, last_y, last_z, shares = weights(turn)
        one_hot = jnp.where(x_index == floor_x, 1.0, 0.0).astype(BF16)
        hot[:, span] = one_hot
        tile_sets = [
            [
                last_y * (hat_z * share),
                hat_y * (last_z * share),
                jnp.where(cell == 0.0, last_y * (last_z * share), 0.0),
            ]
            for share in shares
        ]
        acc_halo[...] += deposited(tile_sets, one_hot)

    outer = settled(acc_halo[...])
    for i in range(3):
        halo_out[i] = outer[i * CELL : (i + 1) * CELL]

    up_y, up_z = lax.rem(my_y + 1, n_py), lax.rem(my_z + 1, n_pz)
    down_y, down_z = lax.rem(my_y + n_py - 1, n_py), lax.rem(my_z + n_pz - 1, n_pz)
    pl.semaphore_wait(barrier, n - 1)
    halos = [
        pltpu.make_async_remote_copy(
            src_ref=halo_out.at[i],
            dst_ref=halo_in.at[i],
            send_sem=halo_send.at[i],
            recv_sem=halo_recv.at[i],
            device_id=target,
            device_id_type=MESH,
        )
        for i, target in enumerate([(up_y, my_z), (my_y, up_z), (up_y, up_z)])
    ]
    for halo in halos:
        halo.start()

    @pl.loop(0, turns)
    def _(turn):
        span, _, hat_y, hat_z, _, _, shares = weights(turn)
        tile_sets = []
        for share in shares:
            scaled = hat_z * share
            tile_sets.append([hat_y[a : a + 1] * scaled for a in range(CELL)])
        acc[...] += deposited(tile_sets, hot[:, span])

    grid = settled(acc[...])
    green = green_factor(rank, n_py, n_pz, nx, nf)
    for load in loads[2:]:
        load.wait()
    for halo in halos:
        halo.wait()

    first = lax.broadcasted_iota(jnp.int32, (CELL, nx), 0) == 0
    beside = halo_in[1]
    doubled = []
    for a in range(CELL):
        tile = grid[a * CELL : (a + 1) * CELL]
        tile = tile + jnp.where(first, beside[a : a + 1], 0.0)
        if a == 0:
            tile = tile + halo_in[0] + jnp.where(first, halo_in[2], 0.0)
        doubled += [tile, tile]
    density = split(jnp.concatenate(doubled, axis=0))
    kept = nx // 2
    both = dot_parts([line[0], line[1]], density, ((1,), (1,)))
    is_real = lax.broadcasted_iota(jnp.int32, (kept, 2 * CELL * CELL), 1) // CELL % 2 == 0
    spectrum = jnp.where(is_real, both[:kept], both[kept:])
    for r in range(n):
        send1[r] = spectrum[r * nf : (r + 1) * nf]

    def exchange(source, target, send_sem, recv_sem):
        @pl.loop(1, n)
        def _(step):
            peer, where = coords(step)
            pltpu.make_async_remote_copy(
                src_ref=source.at[peer],
                dst_ref=target.at[rank],
                send_sem=send_sem,
                recv_sem=recv_sem,
                device_id=where,
                device_id_type=MESH,
            ).start()

        target[rank] = source[rank]
        others = pl.ds(0, n - 1)
        pltpu.make_async_copy(source.at[others], source.at[others], send_sem).wait()
        pltpu.make_async_copy(target.at[others], target.at[others], recv_sem).wait()

    exchange(send1, recv1, send_sem1, recv_sem1)

    for ay in range(n_py):
        for t in range(n_pz // GROUPS):
            tiles = [recv1[ay * n_pz + t * GROUPS + g] for g in range(GROUPS)]
            for a, tile in enumerate(swap_groups(tiles)):
                start = (ay * CELL + a) * nf
                field[start : start + nf, t * 128 : (t + 1) * 128] = tile
    width = 2 * CELL * n_pz

    def plane_transform(values, table):
        count = table.shape[0]
        along = dot_parts(split(values, count), [table[i] for i in range(count)])
        joined = jnp.concatenate([along[:, :width], along[:, width:]], axis=0)
        return dot_parts([rows[i] for i in range(count)], split(joined, count))

    values = field[...]
    row = lax.broadcasted_iota(jnp.int32, values.shape, 0)
    col = lax.broadcasted_iota(jnp.int32, values.shape, 1)
    constant = (row % nf + rank * nf == 0) & (col // CELL % 2 == 0)
    mean = jnp.sum(jnp.where(constant, values, 0.0), axis=0, keepdims=True)
    mean = jnp.sum(mean, axis=1, keepdims=True) * (1.0 / (CELL * CELL * n))
    values = values - jnp.where(constant, mean, 0.0)
    solved = plane_transform(plane_transform(values, fwd) * green, inv)
    for ay in range(n_py):
        for t in range(n_pz // GROUPS):
            tiles = []
            for a in range(CELL):
                start = (ay * CELL + a) * nf
                tiles.append(solved[start : start + nf, t * 128 : (t + 1) * 128])
            for g, tile in enumerate(swap_groups(tiles)):
                send2[ay * n_pz + t * GROUPS + g] = tile

    exchange(send2, recv2, send_sem2, recv_sem2)

    for r in range(n):
        waves[r * nf : (r + 1) * nf] = recv2[r]
    columns = split(jnp.transpose(waves[...]), 3)
    cosines = dot_parts(columns, [line[i, :kept] for i in range(3)])
    sines = dot_parts(columns, [line[i, kept:] for i in range(3)])
    potential = [
        cosines[a * PAIR : a * PAIR + CELL] + sines[a * PAIR + CELL : (a + 1) * PAIR]
        for a in range(CELL)
    ]
    edge_out[0] = potential[CELL - 1]
    edge_out[1] = potential[0]
    edge_out[2] = jnp.concatenate([tile[CELL - 1 : CELL] for tile in potential], axis=0)
    edge_out[3] = jnp.concatenate([tile[0:1] for tile in potential], axis=0)
    edges = [
        pltpu.make_async_remote_copy(
            src_ref=edge_out.at[i],
            dst_ref=edge_in.at[i],
            send_sem=edge_send.at[i],
            recv_sem=edge_recv.at[i],
            device_id=target,
            device_id_type=MESH,
        )
        for i, target in enumerate(
            [(up_y, my_z), (down_y, my_z), (my_y, up_z), (my_y, down_z)]
        )
    ]
    for edge in edges:
        edge.start()
    for a, tile in enumerate(potential):
        pot_ref[a] = tile
    for edge in edges:
        edge.wait()
    side_ref[...] = edge_in[...]


def finish(pot_ref, side_ref, out_hbm, out_ref, sems):
    nx = pot_ref.shape[2]
    copies = []

    def emit(d):
        copies.append(pltpu.make_async_copy(out_ref.at[d], out_hbm.at[d], sems.at[d]))
        copies[-1].start()

    for a in range(CELL):
        tile = pot_ref[a]
        out_ref[2, a] = (pltpu.roll(tile, 1, 1) - pltpu.roll(tile, nx - 1, 1)) * 0.5
    emit(2)
    for a in range(CELL):
        below = pot_ref[a - 1] if a else side_ref[0]
        above = pot_ref[a + 1] if a < CELL - 1 else side_ref[1]
        out_ref[0, a] = (below - above) * 0.5
    emit(0)
    before, after = side_ref[2], side_ref[3]
    lane_row = lax.broadcasted_iota(jnp.int32, (CELL, nx), 0)
    for a in range(CELL):
        tile = pot_ref[a]
        lower = jnp.where(lane_row == 0, before[a : a + 1], pltpu.roll(tile, 1, 0))
        upper = jnp.where(lane_row == CELL - 1, after[a : a + 1], pltpu.roll(tile, CELL - 1, 0))
        out_ref[1, a] = (lower - upper) * 0.5
    emit(1)
    for copy in copies:
        copy.wait()


def solution(mesh):
    n_py, n_pz = mesh.shape["py"], mesh.shape["pz"]
    n = n_py * n_pz
    nx = 512
    nf = nx // 2 // n
    ny, nz = CELL * n_py, CELL * n_pz
    consts = tables(n_py, n_pz, nx, nf)

    def shards(positions, masses):
        chunk = min(positions.shape[1], 2048)
        vmem = pl.BlockSpec(memory_space=pltpu.VMEM)
        hbm = pl.BlockSpec(memory_space=pltpu.HBM)
        block = pltpu.VMEM((n, nf, 128), F32)
        dma = pltpu.SemaphoreType.DMA
        pot, side = pl.pallas_call(
            functools.partial(kernel, n_py, n_pz, nx, nf, chunk),
            out_shape=[pltpu.VMEM((CELL, CELL, nx), F32), pltpu.VMEM((4, CELL, nx), F32)],
            in_specs=[hbm] * 6,
            out_specs=[vmem, vmem],
            scratch_shapes=[
                pltpu.VMEM(positions.shape, F32),
                pltpu.VMEM((1, positions.shape[1]), F32),
                *[pltpu.VMEM(table.shape, BF16) for table in consts],
                dma((6,)),
                pltpu.VMEM((nx, positions.shape[1]), BF16),
                pltpu.VMEM((4 * 3 * CELL, nx), F32),
                pltpu.VMEM((4 * CELL * CELL, nx), F32),
                pltpu.VMEM((3, CELL, nx), F32),
                pltpu.VMEM((3, CELL, nx), F32),
                dma((3,)),
                dma((3,)),
                block,
                block,
                pltpu.VMEM((ny * nf, 2 * nz), F32),
                block,
                block,
                pltpu.VMEM((n * nf, 128), F32),
                dma, dma, dma, dma,
                pltpu.VMEM((4, CELL, nx), F32),
                pltpu.VMEM((4, CELL, nx), F32),
                dma((4,)),
                dma((4,)),
            ],
            compiler_params=pltpu.CompilerParams(
                collective_id=0, has_side_effects=True, vmem_limit_bytes=50 << 20
            ),
        )(*[
            pltpu.with_memory_space_constraint(x, pltpu.HBM)
            for x in (positions, masses.reshape(1, -1), *map(jnp.asarray, consts))
        ])
        return pl.pallas_call(
            finish,
            out_shape=jax.ShapeDtypeStruct((3, CELL, CELL, nx), F32),
            in_specs=[vmem, vmem],
            out_specs=hbm,
            scratch_shapes=[pltpu.VMEM((3, CELL, CELL, nx), F32), dma((3,))],
            compiler_params=pltpu.CompilerParams(vmem_limit_bytes=16 << 20),
        )(pot, side)

    return jax.shard_map(
        shards,
        mesh=mesh,
        in_specs=(P(None, ("py", "pz")), P(("py", "pz"))),
        out_specs=P(None, "py", "pz", None),
        check_vma=False,
    )
```

```python
import functools
import math

import jax
import jax.numpy as jnp
import ml_dtypes
import numpy as np
from jax import lax
from jax.experimental import pallas as pl
from jax.experimental.pallas import tpu as pltpu
from jax.sharding import PartitionSpec as P

MESH = pl.DeviceIdType.MESH
F32 = jnp.float32
BF16 = jnp.bfloat16
SMOOTHING_SQ = 0.25
CELL = 8
CELLS = CELL * CELL
EDGE = 32


def parts(table, count):
    out = []
    for _ in range(count):
        out.append(table.astype(ml_dtypes.bfloat16))
        table = table - out[-1].astype(np.float64)
    return np.stack(out)


def real_form(wave, turned):
    wave = wave * 1j if turned else wave
    return np.block([[wave.real, wave.imag], [-wave.imag, wave.real]])


def tables(n_py, n_pz, nx, nf):
    n = n_py * n_pz
    ny, nz = CELL * n_py, CELL * n_pz
    quarter, half_nf = nx // 4, nf // 2
    along = (2 * np.arange(quarter)[None, :] + np.arange(2)[:, None]).reshape(-1)
    order = np.arange(quarter).reshape(n // 2, 2, half_nf).transpose(1, 0, 2).reshape(-1)
    line, back = [], []
    for odd in range(2):
        waves = 2 * np.arange(quarter) + odd
        phase = (np.outer(waves, along) % nx) * (2 * np.pi / nx)
        line.append(parts(np.concatenate([np.cos(phase), -np.sin(phase)]), 2))
        phase = (np.outer(waves[order], np.arange(nx // 2)) % nx) * (2 * np.pi / nx)
        back.append(parts(np.concatenate([np.cos(phase), -np.sin(phase)]), 3))

    inner = [(a, z) for a in range(CELL) for z in range(CELL)]
    upper = [(CELL, z) for z in range(CELL)] + [(a, CELL) for a in range(CELL)] + [(CELL, CELL)]
    outer = [(-1, z) for z in range(CELL)] + [(CELL, z) for z in range(CELL)]
    outer += [(a, -1) for a in range(CELL)] + [(a, CELL) for a in range(CELL)]
    used = np.zeros(EDGE)
    used[: len(upper)] = 1.0
    upper = np.array(upper + [(0, 0)] * (EDGE - len(upper)))
    inner, outer = np.array(inner), np.array(outer)

    def inside(cells, sign):
        return np.exp(sign * 2j * np.pi * (cells @ np.array(inner).T) / CELL)

    def twiddles(cells, copies):
        p = np.arange(n)
        phase = 2 * np.pi * (
            np.outer(p // n_pz, cells[:, 0]) / ny + np.outer(p % n_pz, cells[:, 1]) / nz
        )
        return np.tile(np.stack([np.cos(phase), np.sin(phase)]), (1, 1, copies))

    share = lambda at: np.where((at == 0) | (at == CELL), 0.5, 1.0)
    flat = share(inner[:, 0]) * share(inner[:, 1])
    flat_edge = share(upper[:, 0]) * share(upper[:, 1]) * used
    pattern = np.zeros((CELL, 256))
    pattern[0, :CELLS] = flat
    pattern[0, 128 : 128 + EDGE] = flat_edge
    turn = np.concatenate([twiddles(inner, 2), twiddles(upper, 4)], axis=2).reshape(2 * n, 256)
    turn = np.concatenate([turn, pattern]).astype(np.float32)
    unturn = np.concatenate([twiddles(inner, 2), twiddles(outer, 4)], axis=2)
    unturn = unturn.reshape(2 * n, 256).astype(np.float32)

    wave = inside(inner, -1)
    fwd = parts(np.concatenate([real_form(wave, 0), real_form(wave, 1)]), 2)
    fwd = np.concatenate([fwd[0], fwd[1]], axis=1)
    wave = inside(upper, -1) * used[:, None]
    spread = [np.kron(np.eye(2), real_form(wave, t)) for t in range(2)]
    fwd_edge = parts(np.concatenate(spread), 2)
    wave, wave_edge = inside(inner, 1).T, inside(outer, 1).T
    pieces = [real_form(wave, 0), real_form(wave, 1)]
    pieces += [np.tile(real_form(wave_edge, t), (1, 2)) for t in range(2)]
    inv = parts(np.concatenate(pieces, axis=1), 2)
    inv = np.concatenate([inv[0], inv[0], inv[1]])
    return np.stack(line), np.stack(back), fwd, fwd_edge, inv, turn, unturn


def plus(a, b):
    return b if a is None else a if b is None else a + b


def minus(a, b):
    return a if b is None else -b if a is None else a - b


def conj(x):
    return x[0], minus(None, x[1]) if x[1] is not None else None


def add(x, y):
    return plus(x[0], y[0]), plus(x[1], y[1])


def sub(x, y):
    return minus(x[0], y[0]), minus(x[1], y[1])


def rotated(x, k, n, sign):
    re, im = x
    if k == 0:
        return x
    if 4 * k == n:
        turned = (minus(None, im) if im is not None else None, re)
        return turned if sign > 0 else (im, -re)
    c, s = math.cos(2 * math.pi * k / n), sign * math.sin(2 * math.pi * k / n)
    if im is None:
        return re * c, re * s
    if 8 * k == n:
        both = (re - im, re + im) if sign > 0 else (re + im, im - re)
        return both[0] * c, both[1] * c
    return re * c - im * s, re * s + im * c


def fft(x, sign):
    n = len(x)
    if n == 1:
        return x
    even, odd = fft(x[::2], sign), fft(x[1::2], sign)
    odd = [rotated(o, k, n, sign) for k, o in enumerate(odd)]
    return [add(e, o) for e, o in zip(even, odd)] + [sub(e, o) for e, o in zip(even, odd)]


def rfft(x):
    n = len(x)
    if n == 1:
        return [(x[0], None)]
    if n == 2:
        return [(x[0] + x[1], None), (x[0] - x[1], None)]
    even, odd = rfft(x[::2]), rfft(x[1::2])
    out = [None] * (n // 2 + 1)
    for k in range(n // 4 + 1):
        turned = rotated(odd[k], k, n, -1)
        out[k] = add(even[k], turned)
        if k < n // 4:
            out[n // 2 - k] = conj(sub(even[k], turned))
    return out


def irfft(x):
    n = 2 * (len(x) - 1)
    if n == 2:
        return [x[0][0] + x[1][0], x[0][0] - x[1][0]]
    even, odd = [], []
    for k in range(n // 4 + 1):
        if 4 * k == n:
            even.append((x[k][0] * 2.0, None))
            odd.append((x[k][1] * -2.0, None) if x[k][1] is not None else (x[k][0] * 0.0, None))
            continue
        mirror = conj(x[n // 2 - k])
        even.append(add(x[k], mirror))
        odd.append(rotated(sub(x[k], mirror), k, n, 1))
    even, odd = irfft(even), irfft(odd)
    return [v for pair in zip(even, odd) for v in pair]


def plane_forward(values, n_py, n_pz):
    lines = [rfft(row) for row in values]
    out = {}
    for pz in range(n_pz // 2 + 1):
        column = [line[pz] for line in lines]
        if all(x[1] is None for x in column):
            found = rfft([x[0] for x in column])
            found += [conj(found[n_py - py]) for py in range(n_py // 2 + 1, n_py)]
        else:
            found = fft(column, -1)
        for py in range(n_py):
            out[py, pz] = found[py]
    return out


def plane_inverse(half, n_py, n_pz):
    columns = []
    for pz in range(n_pz // 2 + 1):
        if pz in (0, n_pz // 2):
            column = irfft([half[py, pz] for py in range(n_py // 2 + 1)])
            columns.append([(x, None) for x in column])
        else:
            columns.append(fft([half[py, pz] for py in range(n_py)], 1))
    return [irfft([column[ay] for column in columns]) for ay in range(n_py)]


def split(x, count=2):
    out = []
    for i in range(count):
        out.append(x.astype(BF16))
        if i < count - 1:
            x = x - out[-1].astype(F32)
    return out


def dot(left, right, dims=((1,), (0,))):
    return lax.dot_general(left, right, (dims, ((), ())), preferred_element_type=F32)


def dot_parts(left, right, dims=((1,), (0,))):
    count = len(left)
    total = None
    for order in reversed(range(count)):
        for i in range(order + 1):
            term = dot(left[i], right[order - i], dims)
            total = term if total is None else total + term
    return total


def green_factor(rank, n_py, n_pz, nx, nf):
    n = n_py * n_pz
    ny, nz = CELL * n_py, CELL * n_pz
    shape = (n * nf, 128)
    row = lax.broadcasted_iota(jnp.int32, shape, 0)
    col = lax.broadcasted_iota(jnp.int32, shape, 1)

    def square(wave, period):
        folded = jnp.minimum(wave, period - wave).astype(F32)
        return (folded * (2.0 * math.pi / period)) ** 2

    p = row // nf
    wave_x = 2 * (lax.rem(rank, n // 2) * nf + row % nf) + rank // (n // 2)
    wave_y = p // n_pz + n_py * (col // CELL % CELL)
    wave_z = p % n_pz + n_pz * (col % CELL)
    total = square(wave_y, ny) + square(wave_z, nz) + square(wave_x, nx)
    safe = jnp.where(total > 0, total, 1.0)
    green = jnp.where(total > 0, -4.0 * math.pi * jnp.exp(-SMOOTHING_SQ * total) / safe, 0.0)
    return green * (jnp.where(wave_x > 0, 1.0, 0.5) * (1.0 / float(ny * nz * nx)))


def kernel(
    n_py, n_pz, nx, nf, chunk,
    pos_hbm, mass_hbm, line_hbm, back_hbm, fwd_hbm, fwd_edge_hbm, inv_hbm, turn_hbm, unturn_hbm,
    pot_ref, side_ref,
    pos_ref, mass_ref, line, back, fwd, fwd_edge, inv, turn, unturn, table_sem,
    acc, green, mixed, send1, recv1, send2, recv2, send_edge, recv_edge, waves_edge,
    send_sem1, recv_sem1, send_sem2, recv_sem2, send_sem3, recv_sem3,
):
    n = n_py * n_pz
    half_nf, half, quarter = nf // 2, nx // 2, nx // 4
    my_y, my_z = lax.axis_index("py"), lax.axis_index("pz")
    rank = my_y * n_pz + my_z

    loads = [
        pltpu.make_async_copy(src, dst, table_sem.at[i])
        for i, (src, dst) in enumerate(
            [
                (pos_hbm, pos_ref),
                (mass_hbm, mass_ref),
                (line_hbm, line),
                (turn_hbm, turn),
                (fwd_hbm, fwd),
                (fwd_edge_hbm, fwd_edge),
                (inv_hbm, inv),
                (unturn_hbm, unturn),
                (back_hbm, back),
            ]
        )
    ]
    for load in loads:
        load.start()

    def coords(step):
        along_z = (n - step) // n_py
        along_z = along_z ^ (2 * (along_z // 4))
        other_y = lax.rem(n - step, n_py) ^ my_y
        other_z = along_z ^ my_z
        return other_y * n_pz + other_z, (other_y, other_z)

    barrier = pltpu.get_barrier_semaphore()

    @pl.loop(1, n)
    def _(step):
        pl.semaphore_signal(barrier, inc=1, device_id=coords(step)[1], device_id_type=MESH)

    base_y = (my_y * CELL).astype(F32)
    base_z = (my_z * CELL).astype(F32)
    row_of = lax.broadcasted_iota(jnp.int32, (CELL, chunk), 0)
    cell = row_of.astype(F32)
    sublane = lax.broadcasted_iota(jnp.int32, (2 * CELL, chunk), 0).astype(F32)

    for load in loads[:2]:
        load.wait()

    def deposited(turn_index):
        span = pl.ds(pl.multiple_of(turn_index * chunk, chunk), chunk)
        along_y = pos_ref[0:1, span] - base_y
        along_z = pos_ref[1:2, span] - base_z
        along_x = pos_ref[2:3, span]
        mass = mass_ref[0:1, span]
        floor_x = jnp.floor(along_x)
        frac_x = along_x - floor_x
        pair = jnp.floor(floor_x * 0.5)
        is_even = floor_x == 2.0 * pair
        lower, upper = mass * (1.0 - frac_x), mass * frac_x
        shares = [
            jnp.where(is_even, lower, 0.0),
            jnp.where(is_even, upper, lower),
            jnp.where(is_even, 0.0, upper),
        ]
        where_x = jnp.broadcast_to(pair, (2 * CELL, chunk)).astype(BF16)
        one_hot = jnp.concatenate(
            [
                jnp.where(
                    where_x == (sublane + float(t)).astype(BF16),
                    jnp.ones((), BF16),
                    jnp.zeros((), BF16),
                )
                for t in range(0, half, 2 * CELL)
            ],
            axis=0,
        )
        hat_y = jnp.maximum(1.0 - jnp.abs(along_y - cell), 0.0)
        hat_z = jnp.maximum(1.0 - jnp.abs(along_z - cell), 0.0)
        last_y = jnp.maximum(along_y - (CELL - 1.0), 0.0)
        last_z = jnp.maximum(along_z - (CELL - 1.0), 0.0)
        tiles = []
        for share in shares:
            scaled = hat_z * share
            tiles += [hat_y[a : a + 1] * scaled for a in range(CELL)]
            tiles += [last_y * scaled, hat_y * (last_z * share)]
        corner = jnp.where(row_of == 0, shares[0], jnp.where(row_of == 1, shares[1], shares[2]))
        tiles.append(jnp.where(row_of < 3, corner * (last_y * last_z), 0.0))
        pair_of = split(jnp.concatenate(tiles, axis=0))
        return dot(jnp.concatenate(pair_of, axis=0), one_hot, ((1,), (1,)))

    turns = pos_ref.shape[1] // chunk
    acc[...] = deposited(0)
    if turns > 1:

        @pl.loop(1, turns)
        def _(turn_index):
            acc[...] += deposited(turn_index)

    for load in loads[2:3]:
        load.wait()
    sums = acc[...]
    rows = sums.shape[0] // 2
    sums = sums[:rows] + sums[rows:]
    block = CELLS + 2 * CELL
    even = sums[:block] + pltpu.roll(sums[2 * block : 3 * block], 1, 1)
    odd = sums[block : 2 * block]
    corner = sums[3 * block :]
    first = lax.broadcasted_iota(jnp.int32, (CELL, half), 0) == 0
    blank = jnp.zeros((CELL, half), F32)
    corner_even = corner + pltpu.roll(pltpu.roll(corner, CELL - 2, 0), 1, 1)
    corner_even = jnp.where(first, corner_even, 0.0)
    corner_odd = jnp.where(first, pltpu.roll(corner, CELL - 1, 0), 0.0)
    even = jnp.concatenate([even, corner_even, blank], axis=0)
    odd = jnp.concatenate([odd, corner_odd, blank], axis=0)

    lane = lax.broadcasted_iota(jnp.int32, (nf, 128), 1)
    is_real = lane < CELLS
    is_real_edge = lane % CELLS < EDGE
    low_half = lax.broadcasted_iota(jnp.int32, (half_nf, 128), 1) < CELLS
    for parity in range(2):
        folded = []
        for grid in (even, odd):
            left, right = grid[:, :quarter], grid[:, quarter:]
            folded.append(left - right if parity else left + right)
        density = [
            jnp.concatenate([x[:CELLS]] * 2 + [x[CELLS:]] * 4, axis=0)
            for x in split(jnp.concatenate(folded, axis=1))
        ]
        both = dot_parts([line[parity, 0], line[parity, 1]], density, ((1,), (1,)))
        for r in range(n // 2):
            re, im = both[r * nf : (r + 1) * nf], both[quarter + r * nf : quarter + (r + 1) * nf]
            peer = parity * (n // 2) + r
            send1[peer, 0:nf] = jnp.where(is_real, re[:, :128], im[:, :128])
            side = jnp.where(is_real_edge, re[:, 128:], im[:, 128:])
            send1[peer, nf : nf + half_nf] = jnp.where(low_half, side[:half_nf], side[half_nf:])

    pl.semaphore_wait(barrier, n - 1)

    def start(source, target, send_sem, recv_sem):
        @pl.loop(1, n)
        def _(step):
            peer, where = coords(step)
            pltpu.make_async_remote_copy(
                src_ref=source.at[peer],
                dst_ref=target.at[rank],
                send_sem=send_sem,
                recv_sem=recv_sem,
                device_id=where,
                device_id_type=MESH,
            ).start()

        target[rank] = source[rank]

    def finish_exchange(source, target, send_sem, recv_sem):
        others = pl.ds(0, n - 1)
        pltpu.make_async_copy(target.at[others], target.at[others], recv_sem).wait()
        pltpu.make_async_copy(source.at[others], source.at[others], send_sem).wait()

    with jax.named_scope("exch1"):
        start(send1, recv1, send_sem1, recv_sem1)
        green[...] = green_factor(rank, n_py, n_pz, nx, nf)
        for load in loads[3:]:
            load.wait()
        with jax.named_scope("wait1"):
            finish_exchange(send1, recv1, send_sem1, recv_sem1)

    def at(ref, row):
        return ref[row : row + 1]

    def every(half_plane, py, pz):
        if pz <= n_pz // 2:
            return half_plane[py, pz], 1
        return half_plane[-py % n_py, n_pz - pz], -1

    turned = []
    for lanes, span, height in (
        (slice(0, 128), slice(0, nf), nf),
        (slice(128, 256), slice(nf, nf + half_nf), half_nf),
    ):
        values = [[recv1[ay * n_pz + az, span] for az in range(n_pz)] for ay in range(n_py)]
        found = plane_forward(values, n_py, n_pz)
        blocks = []
        for p in range(n):
            (re, im), sign = every(found, p // n_pz, p % n_pz)
            c, s = turn[p : p + 1, lanes], turn[n + p : n + p + 1, lanes]
            if im is None:
                u, v = c * re, -(s * re)
            elif sign > 0:
                u, v = c * re + s * im, c * im - s * re
            else:
                u, v = c * re - s * im, -(c * im) - s * re
            blocks.append([u, v])
        turned.append(blocks)
    corner_row = lax.broadcasted_iota(jnp.int32, (half_nf, 128), 0) == 0
    top_row = lax.broadcasted_iota(jnp.int32, (nf, 128), 0) == 0
    level = jnp.sum(turned[0][0][0][0:1] * jnp.where(is_real[0:1], 1.0, 0.0), axis=1, keepdims=True)
    level += jnp.sum(
        turned[1][0][0][0:1] * jnp.where(lane[0:1] < EDGE, 1.0, 0.0), axis=1, keepdims=True
    )
    level = jnp.where(rank == 0, level * (1.0 / CELLS), 0.0)
    flat = turn[2 * n : 2 * n + 1]
    turned[0][0][0] = turned[0][0][0] - jnp.where(top_row, level * flat[:, :128], 0.0)
    turned[1][0][0] = turned[1][0][0] - jnp.where(corner_row, level * flat[:, 128:], 0.0)

    stacked = [
        jnp.concatenate(
            [jnp.concatenate([uv[i] for uv in blocks], axis=0) for i in range(2)], axis=1
        )
        for blocks in turned
    ]
    high, low = split(stacked[0])
    wide = dot(high, fwd[...])
    solved = wide[:, :128] + wide[:, 128:] + dot(low, fwd[:, :128])
    beside = dot_parts(split(stacked[1]), [fwd_edge[0], fwd_edge[1]])
    pieces = []
    for p in range(n):
        rows_of = beside[p * half_nf : (p + 1) * half_nf]
        pieces += [rows_of[:, :128], rows_of[:, 128:]]
    solved = (solved + jnp.concatenate(pieces, axis=0)) * green[...]
    high, low = split(solved)
    mixed[...] = dot(jnp.concatenate([high, low], axis=1), inv[0:256]) + dot(high, inv[256:384])

    for lanes, offset in ((slice(0, 128), 0), (slice(128, 256), 256)):
        ones, twos = {}, {}
        for p in range(n):
            c, s = unturn[p : p + 1, lanes], unturn[n + p : n + p + 1, lanes]
            span = slice(p * nf, (p + 1) * nf)
            y, jy = mixed[span, offset : offset + 128], mixed[span, offset + 128 : offset + 256]
            ones[p // n_pz, p % n_pz] = c * y + s * jy
            twos[p // n_pz, p % n_pz] = c * jy - s * y
        half_plane = {}
        for pz in range(n_pz // 2 + 1):
            for py in range(n_py):
                other = (-py % n_py, -pz % n_pz)
                if other == (py, pz):
                    half_plane[py, pz] = (ones[other] * 2.0, None)
                else:
                    half_plane[py, pz] = (
                        ones[py, pz] + ones[other],
                        twos[other] - twos[py, pz],
                    )
        values = plane_inverse(half_plane, n_py, n_pz)
        for ay in range(n_py):
            for az in range(n_pz):
                value = values[ay][az]
                if offset == 0:
                    send2[ay * n_pz + az] = value
                else:
                    value = jnp.where(low_half, value[:half_nf], value[half_nf:])
                    send_edge[ay * n_pz + az] = value
        if offset == 0:
            start(send2, recv2, send_sem2, recv_sem2)
        else:
            start(send_edge, recv_edge, send_sem3, recv_sem3)

    with jax.named_scope("wait2"):
        finish_exchange(send2, recv2, send_sem2, recv_sem2)

    def potential(columns):
        found = [
            dot_parts(split(columns[parity], 3), [back[parity, i] for i in range(3)])
            for parity in range(2)
        ]
        return found[0] + found[1], found[0] - found[1]

    columns = []
    for parity in range(2):
        peers = range(parity * (n // 2), (parity + 1) * (n // 2))
        rows_of = [
            recv2[r, h * half_nf : (h + 1) * half_nf] for h in range(2) for r in peers
        ]
        turned_back = jnp.transpose(jnp.concatenate(rows_of, axis=0))
        columns.append(jnp.concatenate([turned_back[:CELLS], turned_back[CELLS:]], axis=1))
    left, right = potential(columns)
    for a in range(CELL):
        pot_ref[a, :, :half] = left[a * CELL : (a + 1) * CELL]
        pot_ref[a, :, half:] = right[a * CELL : (a + 1) * CELL]

    with jax.named_scope("wait3"):
        finish_exchange(send_edge, recv_edge, send_sem3, recv_sem3)
    for r in range(n):
        waves_edge[r * half_nf : (r + 1) * half_nf] = recv_edge[r]
    turned_back = jnp.transpose(waves_edge[...])
    columns = []
    for parity in range(2):
        span = slice(parity * CELLS, (parity + 1) * CELLS)
        columns.append(
            jnp.concatenate(
                [
                    turned_back[h * CELLS + c * EDGE : h * CELLS + (c + 1) * EDGE, span]
                    for c in range(2)
                    for h in range(2)
                ],
                axis=1,
            )
        )
    left, right = potential(columns)
    for i in range(4):
        side_ref[i, :, :half] = left[i * CELL : (i + 1) * CELL]
        side_ref[i, :, half:] = right[i * CELL : (i + 1) * CELL]


def finish(pot_ref, side_ref, out_hbm, out_ref, sems):
    nx = pot_ref.shape[2]
    copies = []

    def emit(d):
        copies.append(pltpu.make_async_copy(out_ref.at[d], out_hbm.at[d], sems.at[d]))
        copies[-1].start()

    for a in range(CELL):
        tile = pot_ref[a]
        out_ref[2, a] = (pltpu.roll(tile, 1, 1) - pltpu.roll(tile, nx - 1, 1)) * 0.5
    emit(2)
    for a in range(CELL):
        below = pot_ref[a - 1] if a else side_ref[0]
        above = pot_ref[a + 1] if a < CELL - 1 else side_ref[1]
        out_ref[0, a] = (below - above) * 0.5
    emit(0)
    before, after = side_ref[2], side_ref[3]
    lane_row = lax.broadcasted_iota(jnp.int32, (CELL, nx), 0)
    for a in range(CELL):
        tile = pot_ref[a]
        lower = jnp.where(lane_row == 0, before[a : a + 1], pltpu.roll(tile, 1, 0))
        upper = jnp.where(lane_row == CELL - 1, after[a : a + 1], pltpu.roll(tile, CELL - 1, 0))
        out_ref[1, a] = (lower - upper) * 0.5
    emit(1)
    for copy in copies:
        copy.wait()


def solution(mesh):
    n_py, n_pz = mesh.shape["py"], mesh.shape["pz"]
    n = n_py * n_pz
    nx = 512
    nf = nx // 2 // n
    consts = tables(n_py, n_pz, nx, nf)

    def shards(positions, masses):
        chunk = min(positions.shape[1], 2048)
        vmem = pl.BlockSpec(memory_space=pltpu.VMEM)
        hbm = pl.BlockSpec(memory_space=pltpu.HBM)
        dma = pltpu.SemaphoreType.DMA
        wide = pltpu.VMEM((n, nf + nf // 2, 128), F32)
        block = pltpu.VMEM((n, nf, 128), F32)
        edge = pltpu.VMEM((n, nf // 2, 128), F32)
        operands = [positions, masses.reshape(1, -1), *map(jnp.asarray, consts)]
        pot, side = pl.pallas_call(
            functools.partial(kernel, n_py, n_pz, nx, nf, chunk),
            out_shape=[pltpu.VMEM((CELL, CELL, nx), F32), pltpu.VMEM((4, CELL, nx), F32)],
            in_specs=[hbm] * len(operands),
            out_specs=[vmem, vmem],
            scratch_shapes=[
                *[pltpu.VMEM(x.shape, x.dtype) for x in operands],
                dma((len(operands),)),
                pltpu.VMEM((2 * (3 * (CELLS + 2 * CELL) + CELL), nx // 2), F32),
                pltpu.VMEM((n * nf, 128), F32),
                pltpu.VMEM((n * nf, 512), F32),
                wide, wide, block, block, edge, edge,
                pltpu.VMEM((n * nf // 2, 128), F32),
                dma, dma, dma, dma, dma, dma,
            ],
            compiler_params=pltpu.CompilerParams(
                collective_id=0, has_side_effects=True, vmem_limit_bytes=50 << 20
            ),
        )(*[pltpu.with_memory_space_constraint(x, pltpu.HBM) for x in operands])
        return pl.pallas_call(
            finish,
            out_shape=jax.ShapeDtypeStruct((3, CELL, CELL, nx), F32),
            in_specs=[vmem, vmem],
            out_specs=hbm,
            scratch_shapes=[pltpu.VMEM((3, CELL, CELL, nx), F32), dma((3,))],
            compiler_params=pltpu.CompilerParams(vmem_limit_bytes=16 << 20),
        )(pot, side)

    return jax.shard_map(
        shards,
        mesh=mesh,
        in_specs=(P(None, ("py", "pz")), P(("py", "pz"))),
        out_specs=P(None, "py", "pz", None),
        check_vma=False,
    )
```

```python
import functools
import math

import jax
import jax.numpy as jnp
import ml_dtypes
import numpy as np
from jax import lax
from jax.experimental import pallas as pl
from jax.experimental.pallas import tpu as pltpu
from jax.sharding import PartitionSpec as P

MESH = pl.DeviceIdType.MESH
F32 = jnp.float32
BF16 = jnp.bfloat16
SMOOTHING_SQ = 0.25
CELL = 8
CELLS = CELL * CELL
EDGE = 32


def parts(table, count):
    out = []
    for _ in range(count):
        out.append(table.astype(ml_dtypes.bfloat16))
        table = table - out[-1].astype(np.float64)
    return np.stack(out)


def real_form(wave, turned):
    wave = wave * 1j if turned else wave
    return np.block([[wave.real, wave.imag], [-wave.imag, wave.real]])


def tables(n_py, n_pz, nx, nf):
    n = n_py * n_pz
    ny, nz = CELL * n_py, CELL * n_pz
    quarter, half_nf = nx // 4, nf // 2
    along = (2 * np.arange(quarter)[None, :] + np.arange(2)[:, None]).reshape(-1)
    order = np.arange(quarter).reshape(n // 2, 2, half_nf).transpose(1, 0, 2).reshape(-1)
    line, back = [], []
    for odd in range(2):
        waves = 2 * np.arange(quarter) + odd
        phase = (np.outer(waves, along) % nx) * (2 * np.pi / nx)
        line.append(parts(np.concatenate([np.cos(phase), -np.sin(phase)]), 2))
        phase = (np.outer(waves[order], np.arange(nx // 2)) % nx) * (2 * np.pi / nx)
        back.append(parts(np.concatenate([np.cos(phase), -np.sin(phase)]), 3))

    inner = [(a, z) for a in range(CELL) for z in range(CELL)]
    upper = [(CELL, z) for z in range(CELL)] + [(a, CELL) for a in range(CELL)] + [(CELL, CELL)]
    outer = [(-1, z) for z in range(CELL)] + [(CELL, z) for z in range(CELL)]
    outer += [(a, -1) for a in range(CELL)] + [(a, CELL) for a in range(CELL)]
    used = np.zeros(EDGE)
    used[: len(upper)] = 1.0
    upper = np.array(upper + [(0, 0)] * (EDGE - len(upper)))
    inner, outer = np.array(inner), np.array(outer)

    def inside(cells, sign):
        return np.exp(sign * 2j * np.pi * (cells @ np.array(inner).T) / CELL)

    def twiddles(cells, copies):
        p = np.arange(n)
        phase = 2 * np.pi * (
            np.outer(p // n_pz, cells[:, 0]) / ny + np.outer(p % n_pz, cells[:, 1]) / nz
        )
        return np.tile(np.stack([np.cos(phase), np.sin(phase)]), (1, 1, copies))

    share = lambda at: np.where((at == 0) | (at == CELL), 0.5, 1.0)
    flat = share(inner[:, 0]) * share(inner[:, 1])
    flat_edge = share(upper[:, 0]) * share(upper[:, 1]) * used
    pattern = np.zeros((CELL, 256))
    pattern[0, :CELLS] = flat
    pattern[0, 128 : 128 + EDGE] = flat_edge
    turn = np.concatenate([twiddles(inner, 2), twiddles(upper, 4)], axis=2).reshape(2 * n, 256)
    turn = np.concatenate([turn, pattern]).astype(np.float32)
    unturn = np.concatenate([twiddles(inner, 2), twiddles(outer, 4)], axis=2)
    unturn = unturn.reshape(2 * n, 256).astype(np.float32)

    wave = inside(inner, -1)
    fwd = parts(np.concatenate([real_form(wave, 0), real_form(wave, 1)]), 2)
    fwd = np.concatenate([fwd[0], fwd[1]], axis=1)
    wave = inside(upper, -1) * used[:, None]
    spread = [np.kron(np.eye(2), real_form(wave, t)) for t in range(2)]
    fwd_edge = parts(np.concatenate(spread), 2)
    wave, wave_edge = inside(inner, 1).T, inside(outer, 1).T
    pieces = [real_form(wave, 0), real_form(wave, 1)]
    pieces += [np.tile(real_form(wave_edge, t), (1, 2)) for t in range(2)]
    inv = parts(np.concatenate(pieces, axis=1), 2)
    inv = np.concatenate([inv[0], inv[0], inv[1]])
    return np.stack(line), np.stack(back), fwd, fwd_edge, inv, turn, unturn


def plus(a, b):
    return b if a is None else a if b is None else a + b


def minus(a, b):
    return a if b is None else -b if a is None else a - b


def conj(x):
    return x[0], minus(None, x[1]) if x[1] is not None else None


def add(x, y):
    return plus(x[0], y[0]), plus(x[1], y[1])


def sub(x, y):
    return minus(x[0], y[0]), minus(x[1], y[1])


def rotated(x, k, n, sign):
    re, im = x
    if k == 0:
        return x
    if 4 * k == n:
        turned = (minus(None, im) if im is not None else None, re)
        return turned if sign > 0 else (im, -re)
    c, s = math.cos(2 * math.pi * k / n), sign * math.sin(2 * math.pi * k / n)
    if im is None:
        return re * c, re * s
    if 8 * k == n:
        both = (re - im, re + im) if sign > 0 else (re + im, im - re)
        return both[0] * c, both[1] * c
    return re * c - im * s, re * s + im * c


def fft(x, sign):
    n = len(x)
    if n == 1:
        return x
    even, odd = fft(x[::2], sign), fft(x[1::2], sign)
    odd = [rotated(o, k, n, sign) for k, o in enumerate(odd)]
    return [add(e, o) for e, o in zip(even, odd)] + [sub(e, o) for e, o in zip(even, odd)]


def rfft(x):
    n = len(x)
    if n == 1:
        return [(x[0], None)]
    if n == 2:
        return [(x[0] + x[1], None), (x[0] - x[1], None)]
    even, odd = rfft(x[::2]), rfft(x[1::2])
    out = [None] * (n // 2 + 1)
    for k in range(n // 4 + 1):
        turned = rotated(odd[k], k, n, -1)
        out[k] = add(even[k], turned)
        if k < n // 4:
            out[n // 2 - k] = conj(sub(even[k], turned))
    return out


def irfft(x):
    n = 2 * (len(x) - 1)
    if n == 2:
        return [x[0][0] + x[1][0], x[0][0] - x[1][0]]
    even, odd = [], []
    for k in range(n // 4 + 1):
        if 4 * k == n:
            even.append((x[k][0] * 2.0, None))
            odd.append((x[k][1] * -2.0, None) if x[k][1] is not None else (x[k][0] * 0.0, None))
            continue
        mirror = conj(x[n // 2 - k])
        even.append(add(x[k], mirror))
        odd.append(rotated(sub(x[k], mirror), k, n, 1))
    even, odd = irfft(even), irfft(odd)
    return [v for pair in zip(even, odd) for v in pair]


def plane_forward(values, n_py, n_pz):
    lines = [rfft(row) for row in values]
    out = {}
    for pz in range(n_pz // 2 + 1):
        column = [line[pz] for line in lines]
        if all(x[1] is None for x in column):
            found = rfft([x[0] for x in column])
            found += [conj(found[n_py - py]) for py in range(n_py // 2 + 1, n_py)]
        else:
            found = fft(column, -1)
        for py in range(n_py):
            out[py, pz] = found[py]
    return out


def plane_inverse(half, n_py, n_pz):
    columns = []
    for pz in range(n_pz // 2 + 1):
        if pz in (0, n_pz // 2):
            column = irfft([half[py, pz] for py in range(n_py // 2 + 1)])
            columns.append([(x, None) for x in column])
        else:
            columns.append(fft([half[py, pz] for py in range(n_py)], 1))
    return [irfft([column[ay] for column in columns]) for ay in range(n_py)]


def split(x, count=2):
    out = []
    for i in range(count):
        out.append(x.astype(BF16))
        if i < count - 1:
            x = x - out[-1].astype(F32)
    return out


def dot(left, right, dims=((1,), (0,))):
    return lax.dot_general(left, right, (dims, ((), ())), preferred_element_type=F32)


def dot_parts(left, right, dims=((1,), (0,))):
    count = len(left)
    total = None
    for order in reversed(range(count)):
        for i in range(order + 1):
            term = dot(left[i], right[order - i], dims)
            total = term if total is None else total + term
    return total


def green_factor(owner, parity, n_py, n_pz, nx, nf):
    n = n_py * n_pz
    ny, nz = CELL * n_py, CELL * n_pz
    shape = (n * nf, 128)
    row = lax.broadcasted_iota(jnp.int32, shape, 0)
    col = lax.broadcasted_iota(jnp.int32, shape, 1)

    def square(wave, period):
        folded = jnp.minimum(wave, period - wave).astype(F32)
        return (folded * (2.0 * math.pi / period)) ** 2

    p = row // nf
    wave_x = 2 * (owner * nf + row % nf) + parity
    wave_y = p // n_pz + n_py * (col // CELL % CELL)
    wave_z = p % n_pz + n_pz * (col % CELL)
    total = square(wave_y, ny) + square(wave_z, nz) + square(wave_x, nx)
    safe = jnp.where(total > 0, total, 1.0)
    green = jnp.where(total > 0, -4.0 * math.pi * jnp.exp(-SMOOTHING_SQ * total) / safe, 0.0)
    return green * (jnp.where(wave_x > 0, 1.0, 0.5) * (1.0 / float(ny * nz * nx)))


def kernel(
    n_py, n_pz, nx, nf, chunk,
    pos_hbm, mass_hbm, line_hbm, back_hbm, fwd_hbm, fwd_edge_hbm, inv_hbm, turn_hbm, unturn_hbm,
    pot_ref, side_ref,
    pos_ref, mass_ref, line, back, fwd, fwd_edge, inv, turn, unturn, table_sem,
    acc, green, mixed, send1, recv1, send2, recv2, waves_edge,
    send_sem1, recv_sem1, send_sem2, recv_sem2,
):
    n = n_py * n_pz
    half_nf, half, quarter = nf // 2, nx // 2, nx // 4
    my_y, my_z = lax.axis_index("py"), lax.axis_index("pz")
    rank = my_y * n_pz + my_z

    loads = [
        pltpu.make_async_copy(src, dst, table_sem.at[i])
        for i, (src, dst) in enumerate(
            [
                (pos_hbm, pos_ref),
                (mass_hbm, mass_ref),
                (line_hbm, line),
                (turn_hbm, turn),
                (fwd_hbm, fwd),
                (fwd_edge_hbm, fwd_edge),
                (inv_hbm, inv),
                (unturn_hbm, unturn),
                (back_hbm, back),
            ]
        )
    ]
    for load in loads[:2]:
        load.start()

    n_own, half_z, first_z = n // 2, n_pz // 2, n_pz // 4
    own_z = my_z - first_z
    is_owner = (own_z >= 0) & (own_z < half_z)
    is_guest = jnp.logical_not(is_owner)
    owner = my_y * half_z + own_z
    turn_z = jnp.where(my_z >= half_z, first_z, 0) ^ lax.rem(my_z, 2)

    def far_first(step):
        along = step % n_pz
        return -(along // 4), -bin(step).count("1"), along % 4 // 2, -step

    everyone, owners = [], []
    for step in sorted(range(1, n), key=far_first):
        other_y, other_z = (step // n_pz) ^ my_y, (step % n_pz) ^ my_z
        everyone.append((other_y * n_pz + other_z, (other_y, other_z)))
    for step in sorted(range(n_own), key=lambda v: (-(v % half_z // 2), -bin(v // half_z).count("1"))):
        other_y, other_z = (step // half_z) ^ my_y, (step % half_z) ^ turn_z
        place = (other_y, other_z + first_z)
        owners.append((step < half_z, other_y * half_z + other_z, place))

    barrier = pltpu.get_barrier_semaphore()

    @pl.when(is_owner)
    def _():
        for _, where in everyone:
            pl.semaphore_signal(barrier, inc=1, device_id=where, device_id_type=MESH)

    @pl.when(is_guest)
    def _():
        for _, _, where in owners:
            pl.semaphore_signal(barrier, inc=1, device_id=where, device_id_type=MESH)


    for load in loads[2:]:
        load.start()
    base_y = (my_y * CELL).astype(F32)
    base_z = (my_z * CELL).astype(F32)
    row_of = lax.broadcasted_iota(jnp.int32, (CELL, chunk), 0)
    cell = row_of.astype(F32)
    sublane = lax.broadcasted_iota(jnp.int32, (2 * CELL, chunk), 0).astype(F32)

    for load in loads[:2]:
        load.wait()

    def deposited(turn_index):
        span = pl.ds(pl.multiple_of(turn_index * chunk, chunk), chunk)
        tall = (CELL, chunk)
        along_y = jnp.broadcast_to(pos_ref[0:1, span], tall) - base_y
        along_z = jnp.broadcast_to(pos_ref[1:2, span], tall) - base_z
        along_x = jnp.broadcast_to(pos_ref[2:3, span], tall)
        mass = jnp.broadcast_to(mass_ref[0:1, span], tall)
        floor_x = jnp.floor(along_x)
        pair = jnp.floor(along_x * 0.5)
        is_even = floor_x == 2.0 * pair
        upper = mass * (along_x - floor_x)
        lower = mass * (1.0 - (along_x - floor_x))
        shares = [
            jnp.where(is_even, lower, 0.0),
            jnp.where(is_even, upper, lower),
            jnp.where(is_even, 0.0, upper),
        ]
        where_x = jnp.concatenate([pair, pair], axis=0).astype(BF16)
        one_hot = jnp.concatenate(
            [
                jnp.where(
                    where_x == (sublane + float(t)).astype(BF16),
                    jnp.ones((), BF16),
                    jnp.zeros((), BF16),
                )
                for t in range(0, half, 2 * CELL)
            ],
            axis=0,
        )
        hat_y = jnp.maximum(1.0 - jnp.abs(along_y - cell), 0.0)
        hat_z = jnp.maximum(1.0 - jnp.abs(along_z - cell), 0.0)
        last_y = jnp.maximum(along_y - (CELL - 1.0), 0.0)
        last_z = jnp.maximum(along_z - (CELL - 1.0), 0.0)
        tiles = []
        for share in shares:
            scaled = hat_z * share
            tiles += [hat_y[a : a + 1] * scaled for a in range(CELL)]
            tiles += [last_y * scaled, hat_y * (last_z * share)]
        corner = jnp.where(row_of == 0, shares[0], jnp.where(row_of == 1, shares[1], shares[2]))
        tiles.append(jnp.where(row_of < 3, corner * (last_y * last_z), 0.0))
        tiles.append(jnp.zeros(tall, F32))
        return split(jnp.concatenate(tiles, axis=0)), one_hot

    turns = pos_ref.shape[1] // chunk

    acc[...] = jnp.zeros_like(acc)

    @pl.loop(0, turns)
    def _(index):
        masses, one_hot = deposited(index)
        for i in range(2):
            acc[i] += dot(masses[i], one_hot, ((1,), (1,)))

    for load in loads[2:3]:
        load.wait()
    sums = acc[0] + acc[1]
    block = CELLS + 2 * CELL
    even = sums[:block] + pltpu.roll(sums[2 * block : 3 * block], 1, 1)
    odd = sums[block : 2 * block]
    corner = sums[3 * block : 3 * block + CELL]
    first = lax.broadcasted_iota(jnp.int32, (CELL, half), 0) == 0
    blank = jnp.zeros((CELL, half), F32)
    corner_even = corner + pltpu.roll(pltpu.roll(corner, CELL - 2, 0), 1, 1)
    corner_even = jnp.where(first, corner_even, 0.0)
    corner_odd = jnp.where(first, pltpu.roll(corner, CELL - 1, 0), 0.0)
    even = jnp.concatenate([even, corner_even, blank], axis=0)
    odd = jnp.concatenate([odd, corner_odd, blank], axis=0)

    lane = lax.broadcasted_iota(jnp.int32, (nf, 128), 1)
    is_real = lane < CELLS
    is_real_edge = lane % CELLS < EDGE
    low_half = lax.broadcasted_iota(jnp.int32, (half_nf, 128), 1) < CELLS
    for parity in range(2):
        folded = []
        for grid in (even, odd):
            left, right = grid[:, :quarter], grid[:, quarter:]
            folded.append(left - right if parity else left + right)
        density = [
            jnp.concatenate([x[:CELLS]] * 2 + [x[CELLS:]] * 4, axis=0)
            for x in split(jnp.concatenate(folded, axis=1))
        ]
        both = dot_parts([line[parity, 0], line[parity, 1]], density, ((1,), (1,)))
        for r in range(n_own):
            re, im = both[r * nf : (r + 1) * nf], both[quarter + r * nf : quarter + (r + 1) * nf]
            send1[parity, r, 0:nf] = jnp.where(is_real, re[:, :128], im[:, :128])
            side = jnp.where(is_real_edge, re[:, 128:], im[:, 128:])
            send1[parity, r, nf : nf + half_nf] = jnp.where(
                low_half, side[:half_nf], side[half_nf:]
            )
        if parity == 0:

            @pl.when(is_owner)
            def _():
                pl.semaphore_wait(barrier, n - 1)

            @pl.when(is_guest)
            def _():
                pl.semaphore_wait(barrier, n_own)

        for maybe_self, peer, where in owners:
            copy = pltpu.make_async_remote_copy(
                src_ref=send1.at[parity, peer],
                dst_ref=recv1.at[parity, rank],
                send_sem=send_sem1.at[parity],
                recv_sem=recv_sem1.at[parity],
                device_id=where,
                device_id_type=MESH,
            )
            if maybe_self:
                pl.when(where[1] != my_z)(copy.start)
            else:
                copy.start()

    def wait_for(ref, parity, count, sem):
        span = ref.at[parity, pl.ds(0, count)]
        pltpu.make_async_copy(span, span, sem.at[parity]).wait()

    def every(half_plane, py, pz):
        if pz <= n_pz // 2:
            return half_plane[py, pz], 1
        return half_plane[-py % n_py, n_pz - pz], -1

    def middle(parity):
        turned = []
        for lanes, span, height in (
            (slice(0, 128), slice(0, nf), nf),
            (slice(128, 256), slice(nf, nf + half_nf), half_nf),
        ):
            values = [[recv1[parity, ay * n_pz + az, span] for az in range(n_pz)] for ay in range(n_py)]
            found = plane_forward(values, n_py, n_pz)
            blocks = []
            for p in range(n):
                (re, im), sign = every(found, p // n_pz, p % n_pz)
                c, s = turn[p : p + 1, lanes], turn[n + p : n + p + 1, lanes]
                if im is None:
                    u, v = c * re, -(s * re)
                elif sign > 0:
                    u, v = c * re + s * im, c * im - s * re
                else:
                    u, v = c * re - s * im, -(c * im) - s * re
                blocks.append([u, v])
            turned.append(blocks)
        if parity == 0:
            corner_row = lax.broadcasted_iota(jnp.int32, (half_nf, 128), 0) == 0
            top_row = lax.broadcasted_iota(jnp.int32, (nf, 128), 0) == 0
            level = jnp.sum(turned[0][0][0][0:1] * jnp.where(is_real[0:1], 1.0, 0.0), axis=1, keepdims=True)
            level += jnp.sum(
                turned[1][0][0][0:1] * jnp.where(lane[0:1] < EDGE, 1.0, 0.0), axis=1, keepdims=True
            )
            level = jnp.where(owner == 0, level * (1.0 / CELLS), 0.0)
            flat = turn[2 * n : 2 * n + 1]
            turned[0][0][0] = turned[0][0][0] - jnp.where(top_row, level * flat[:, :128], 0.0)
            turned[1][0][0] = turned[1][0][0] - jnp.where(corner_row, level * flat[:, 128:], 0.0)

        stacked = [
            jnp.concatenate(
                [jnp.concatenate([uv[i] for uv in blocks], axis=0) for i in range(2)], axis=1
            )
            for blocks in turned
        ]
        high, low = split(stacked[0])
        wide = dot(high, fwd[...])
        solved = wide[:, :128] + wide[:, 128:] + dot(low, fwd[:, :128])
        beside = dot_parts(split(stacked[1]), [fwd_edge[0], fwd_edge[1]])
        pieces = []
        for p in range(n):
            rows_of = beside[p * half_nf : (p + 1) * half_nf]
            pieces += [rows_of[:, :128], rows_of[:, 128:]]
        solved = (solved + jnp.concatenate(pieces, axis=0)) * green[parity]
        high, low = split(solved)
        mixed[...] = dot(jnp.concatenate([high, low], axis=1), inv[0:256]) + dot(high, inv[256:384])

        for lanes, offset in ((slice(0, 128), 0), (slice(128, 256), 256)):
            ones, twos = {}, {}
            for p in range(n):
                c, s = unturn[p : p + 1, lanes], unturn[n + p : n + p + 1, lanes]
                span = slice(p * nf, (p + 1) * nf)
                y, jy = mixed[span, offset : offset + 128], mixed[span, offset + 128 : offset + 256]
                ones[p // n_pz, p % n_pz] = c * y + s * jy
                twos[p // n_pz, p % n_pz] = c * jy - s * y
            half_plane = {}
            for pz in range(n_pz // 2 + 1):
                for py in range(n_py):
                    other = (-py % n_py, -pz % n_pz)
                    if other == (py, pz):
                        half_plane[py, pz] = (ones[other] * 2.0, None)
                    else:
                        half_plane[py, pz] = (
                            ones[py, pz] + ones[other],
                            twos[other] - twos[py, pz],
                        )
            values = plane_inverse(half_plane, n_py, n_pz)
            for ay in range(n_py):
                for az in range(n_pz):
                    value = values[ay][az]
                    if offset == 0:
                        send2[parity, ay * n_pz + az, 0:nf] = value
                    else:
                        value = jnp.where(low_half, value[:half_nf], value[half_nf:])
                        send2[parity, ay * n_pz + az, nf : nf + half_nf] = value
        for peer, where in everyone:
            pltpu.make_async_remote_copy(
                src_ref=send2.at[parity, peer],
                dst_ref=recv2.at[parity, owner],
                send_sem=send_sem2.at[parity],
                recv_sem=recv_sem2.at[parity],
                device_id=where,
                device_id_type=MESH,
            ).start()
        recv2[parity, owner] = send2[parity, rank]

    @pl.when(is_owner)
    def _():
        for parity in range(2):
            recv1[parity, rank] = send1[parity, owner]
            green[parity] = green_factor(owner, parity, n_py, n_pz, nx, nf)
        for load in loads[3:8]:
            load.wait()
        for parity in range(2):
            with jax.named_scope("wait1"):
                wait_for(recv1, parity, n - 1, recv_sem1)
            with jax.named_scope("mid"):
                middle(parity)

    @pl.when(is_guest)
    def _():
        for load in loads[3:8]:
            load.wait()

    loads[8].wait()
    found = []
    for parity in range(2):
        with jax.named_scope("wait2"):

            @pl.when(is_owner)
            def _():
                wait_for(recv2, parity, n_own - 1, recv_sem2)

            @pl.when(is_guest)
            def _():
                wait_for(recv2, parity, n_own, recv_sem2)

        for r in range(n_own):
            waves_edge[r * half_nf : (r + 1) * half_nf] = recv2[parity, r, nf : nf + half_nf]
        beside = jnp.transpose(waves_edge[...])
        rows_of = [
            recv2[parity, r, h * half_nf : (h + 1) * half_nf]
            for h in range(2)
            for r in range(n_own)
        ]
        inner = jnp.transpose(jnp.concatenate(rows_of, axis=0))
        columns = []
        for c in range(2):
            pieces = [
                beside[h * CELLS + c * EDGE : h * CELLS + (c + 1) * EDGE] for h in range(2)
            ]
            columns.append(
                jnp.concatenate(
                    [inner[c * CELLS : (c + 1) * CELLS], jnp.concatenate(pieces, axis=1)], axis=0
                )
            )
        found.append(
            dot_parts(
                split(jnp.concatenate(columns, axis=1), 3), [back[parity, i] for i in range(3)]
            )
        )
    for side, value in enumerate((found[0] + found[1], found[0] - found[1])):
        span = slice(side * half, (side + 1) * half)
        for a in range(CELL):
            pot_ref[a, :, span] = value[a * CELL : (a + 1) * CELL]
        for i in range(4):
            side_ref[i, :, span] = value[CELLS + i * CELL : CELLS + (i + 1) * CELL]

    @pl.when(is_owner)
    def _():
        for parity in range(2):
            wait_for(send1, parity, n_own - 1, send_sem1)
            wait_for(send2, parity, n - 1, send_sem2)

    @pl.when(is_guest)
    def _():
        for parity in range(2):
            wait_for(send1, parity, n_own, send_sem1)


def finish(pot_ref, side_ref, out_hbm, out_ref, sems):
    nx = pot_ref.shape[2]
    copies = []

    def emit(d):
        copies.append(pltpu.make_async_copy(out_ref.at[d], out_hbm.at[d], sems.at[d]))
        copies[-1].start()

    for a in range(CELL):
        tile = pot_ref[a]
        out_ref[2, a] = (pltpu.roll(tile, 1, 1) - pltpu.roll(tile, nx - 1, 1)) * 0.5
    emit(2)
    for a in range(CELL):
        below = pot_ref[a - 1] if a else side_ref[0]
        above = pot_ref[a + 1] if a < CELL - 1 else side_ref[1]
        out_ref[0, a] = (below - above) * 0.5
    emit(0)
    before, after = side_ref[2], side_ref[3]
    lane_row = lax.broadcasted_iota(jnp.int32, (CELL, nx), 0)
    for a in range(CELL):
        tile = pot_ref[a]
        lower = jnp.where(lane_row == 0, before[a : a + 1], pltpu.roll(tile, 1, 0))
        upper = jnp.where(lane_row == CELL - 1, after[a : a + 1], pltpu.roll(tile, CELL - 1, 0))
        out_ref[1, a] = (lower - upper) * 0.5
    emit(1)
    for copy in copies:
        copy.wait()


def solution(mesh):
    n_py, n_pz = mesh.shape["py"], mesh.shape["pz"]
    n = n_py * n_pz
    nx = 512
    nf = nx // 4 // (n // 2)
    consts = tables(n_py, n_pz, nx, nf)

    def shards(positions, masses):
        chunk = min(positions.shape[1], 2048)
        vmem = pl.BlockSpec(memory_space=pltpu.VMEM)
        hbm = pl.BlockSpec(memory_space=pltpu.HBM)
        dma = pltpu.SemaphoreType.DMA
        rows = nf + nf // 2
        few, all_of = (pltpu.VMEM((2, count, rows, 128), F32) for count in (n // 2, n))
        operands = [positions, masses.reshape(1, -1), *map(jnp.asarray, consts)]
        pot, side = pl.pallas_call(
            functools.partial(kernel, n_py, n_pz, nx, nf, chunk),
            out_shape=[pltpu.VMEM((CELL, CELL, nx), F32), pltpu.VMEM((4, CELL, nx), F32)],
            in_specs=[hbm] * len(operands),
            out_specs=[vmem, vmem],
            scratch_shapes=[
                *[pltpu.VMEM(x.shape, x.dtype) for x in operands],
                dma((len(operands),)),
                pltpu.VMEM((2, 3 * (CELLS + 2 * CELL) + 2 * CELL, nx // 2), F32),
                pltpu.VMEM((2, n * nf, 128), F32),
                pltpu.VMEM((n * nf, 512), F32),
                few, all_of, all_of, few,
                pltpu.VMEM((n // 2 * (nf // 2), 128), F32),
                dma((2,)), dma((2,)), dma((2,)), dma((2,)),
            ],
            compiler_params=pltpu.CompilerParams(
                collective_id=0, has_side_effects=True, vmem_limit_bytes=50 << 20
            ),
        )(*[pltpu.with_memory_space_constraint(x, pltpu.HBM) for x in operands])
        return pl.pallas_call(
            finish,
            out_shape=jax.ShapeDtypeStruct((3, CELL, CELL, nx), F32),
            in_specs=[vmem, vmem],
            out_specs=hbm,
            scratch_shapes=[pltpu.VMEM((3, CELL, CELL, nx), F32), dma((3,))],
            compiler_params=pltpu.CompilerParams(vmem_limit_bytes=16 << 20),
        )(pot, side)

    return jax.shard_map(
        shards,
        mesh=mesh,
        in_specs=(P(None, ("py", "pz")), P(("py", "pz"))),
        out_specs=P(None, "py", "pz", None),
        check_vma=False,
    )
```

```python
import functools
import math

import jax
import jax.numpy as jnp
import ml_dtypes
import numpy as np
from jax import lax
from jax.experimental import pallas as pl
from jax.experimental.pallas import tpu as pltpu
from jax.sharding import PartitionSpec as P

MESH = pl.DeviceIdType.MESH
F32 = jnp.float32
BF16 = jnp.bfloat16
SMOOTHING_SQ = 0.25
CELL = 8
CELLS = CELL * CELL
EDGE = 32


def parts(table, count):
    out = []
    for _ in range(count):
        out.append(table.astype(ml_dtypes.bfloat16))
        table = table - out[-1].astype(np.float64)
    return np.stack(out)


def real_form(wave, turned):
    wave = wave * 1j if turned else wave
    return np.block([[wave.real, wave.imag], [-wave.imag, wave.real]])


def tables(n_py, n_pz, nx, nf):
    n = n_py * n_pz
    ny, nz = CELL * n_py, CELL * n_pz
    quarter, half_nf = nx // 4, nf // 2
    along = (2 * np.arange(quarter)[None, :] + np.arange(2)[:, None]).reshape(-1)
    order = np.arange(quarter).reshape(n // 2, 2, half_nf).transpose(1, 0, 2).reshape(-1)
    line, back = [], []
    for odd in range(2):
        waves = 2 * np.arange(quarter) + odd
        phase = (np.outer(waves, along) % nx) * (2 * np.pi / nx)
        line.append(parts(np.concatenate([np.cos(phase), -np.sin(phase)]), 2))
        phase = (np.outer(waves[order], np.arange(nx // 2)) % nx) * (2 * np.pi / nx)
        back.append(parts(np.concatenate([np.cos(phase), -np.sin(phase)]), 3))

    inner = [(a, z) for a in range(CELL) for z in range(CELL)]
    upper = [(CELL, z) for z in range(CELL)] + [(a, CELL) for a in range(CELL)] + [(CELL, CELL)]
    outer = [(-1, z) for z in range(CELL)] + [(CELL, z) for z in range(CELL)]
    outer += [(a, -1) for a in range(CELL)] + [(a, CELL) for a in range(CELL)]
    used = np.zeros(EDGE)
    used[: len(upper)] = 1.0
    upper = np.array(upper + [(0, 0)] * (EDGE - len(upper)))
    inner, outer = np.array(inner), np.array(outer)

    def inside(cells, sign):
        return np.exp(sign * 2j * np.pi * (cells @ np.array(inner).T) / CELL)

    def twiddles(cells, copies):
        p = np.arange(n)
        phase = 2 * np.pi * (
            np.outer(p // n_pz, cells[:, 0]) / ny + np.outer(p % n_pz, cells[:, 1]) / nz
        )
        return np.tile(np.stack([np.cos(phase), np.sin(phase)]), (1, 1, copies))

    share = lambda at: np.where((at == 0) | (at == CELL), 0.5, 1.0)
    flat = share(inner[:, 0]) * share(inner[:, 1])
    flat_edge = share(upper[:, 0]) * share(upper[:, 1]) * used
    pattern = np.zeros((CELL, 256))
    pattern[0, :CELLS] = flat
    pattern[0, 128 : 128 + EDGE] = flat_edge
    turn = np.concatenate([twiddles(inner, 2), twiddles(upper, 4)], axis=2).reshape(2 * n, 256)
    turn = np.concatenate([turn, pattern]).astype(np.float32)
    unturn = np.concatenate([twiddles(inner, 2), twiddles(outer, 4)], axis=2)
    unturn = unturn.reshape(2 * n, 256).astype(np.float32)

    wave = inside(inner, -1)
    fwd = parts(np.concatenate([real_form(wave, 0), real_form(wave, 1)]), 2)
    fwd = np.concatenate([fwd[0], fwd[1]], axis=1)
    wave = inside(upper, -1) * used[:, None]
    spread = [np.kron(np.eye(2), real_form(wave, t)) for t in range(2)]
    fwd_edge = parts(np.concatenate(spread), 2)
    wave, wave_edge = inside(inner, 1).T, inside(outer, 1).T
    pieces = [real_form(wave, 0), real_form(wave, 1)]
    pieces += [np.tile(real_form(wave_edge, t), (1, 2)) for t in range(2)]
    inv = parts(np.concatenate(pieces, axis=1), 2)
    inv = np.concatenate([inv[0], inv[0], inv[1]])
    return np.stack(line), np.stack(back), fwd, fwd_edge, inv, turn, unturn


def plus(a, b):
    return b if a is None else a if b is None else a + b


def minus(a, b):
    return a if b is None else -b if a is None else a - b


def conj(x):
    return x[0], minus(None, x[1]) if x[1] is not None else None


def add(x, y):
    return plus(x[0], y[0]), plus(x[1], y[1])


def sub(x, y):
    return minus(x[0], y[0]), minus(x[1], y[1])


def rotated(x, k, n, sign):
    re, im = x
    if k == 0:
        return x
    if 4 * k == n:
        turned = (minus(None, im) if im is not None else None, re)
        return turned if sign > 0 else (im, -re)
    c, s = math.cos(2 * math.pi * k / n), sign * math.sin(2 * math.pi * k / n)
    if im is None:
        return re * c, re * s
    if 8 * k == n:
        both = (re - im, re + im) if sign > 0 else (re + im, im - re)
        return both[0] * c, both[1] * c
    return re * c - im * s, re * s + im * c


def fft(x, sign):
    n = len(x)
    if n == 1:
        return x
    even, odd = fft(x[::2], sign), fft(x[1::2], sign)
    odd = [rotated(o, k, n, sign) for k, o in enumerate(odd)]
    return [add(e, o) for e, o in zip(even, odd)] + [sub(e, o) for e, o in zip(even, odd)]


def rfft(x):
    n = len(x)
    if n == 1:
        return [(x[0], None)]
    if n == 2:
        return [(x[0] + x[1], None), (x[0] - x[1], None)]
    even, odd = rfft(x[::2]), rfft(x[1::2])
    out = [None] * (n // 2 + 1)
    for k in range(n // 4 + 1):
        turned = rotated(odd[k], k, n, -1)
        out[k] = add(even[k], turned)
        if k < n // 4:
            out[n // 2 - k] = conj(sub(even[k], turned))
    return out


def irfft(x):
    n = 2 * (len(x) - 1)
    if n == 2:
        return [x[0][0] + x[1][0], x[0][0] - x[1][0]]
    even, odd = [], []
    for k in range(n // 4 + 1):
        if 4 * k == n:
            even.append((x[k][0] * 2.0, None))
            odd.append((x[k][1] * -2.0, None) if x[k][1] is not None else (x[k][0] * 0.0, None))
            continue
        mirror = conj(x[n // 2 - k])
        even.append(add(x[k], mirror))
        odd.append(rotated(sub(x[k], mirror), k, n, 1))
    even, odd = irfft(even), irfft(odd)
    return [v for pair in zip(even, odd) for v in pair]


def plane_forward(values, n_py, n_pz):
    lines = [rfft(row) for row in values]
    out = {}
    for pz in range(n_pz // 2 + 1):
        column = [line[pz] for line in lines]
        if all(x[1] is None for x in column):
            found = rfft([x[0] for x in column])
            found += [conj(found[n_py - py]) for py in range(n_py // 2 + 1, n_py)]
        else:
            found = fft(column, -1)
        for py in range(n_py):
            out[py, pz] = found[py]
    return out


def plane_inverse(half, n_py, n_pz):
    columns = []
    for pz in range(n_pz // 2 + 1):
        if pz in (0, n_pz // 2):
            column = irfft([half[py, pz] for py in range(n_py // 2 + 1)])
            columns.append([(x, None) for x in column])
        else:
            columns.append(fft([half[py, pz] for py in range(n_py)], 1))
    return [irfft([column[ay] for column in columns]) for ay in range(n_py)]


def split(x, count=2):
    out = []
    for i in range(count):
        out.append(x.astype(BF16))
        if i < count - 1:
            x = x - out[-1].astype(F32)
    return out


def dot(left, right, dims=((1,), (0,))):
    return lax.dot_general(left, right, (dims, ((), ())), preferred_element_type=F32)


def dot_parts(left, right, dims=((1,), (0,))):
    count = len(left)
    total = None
    for order in reversed(range(count)):
        for i in range(order + 1):
            term = dot(left[i], right[order - i], dims)
            total = term if total is None else total + term
    return total


def green_factor(owner, parity, n_py, n_pz, nx, nf):
    n = n_py * n_pz
    ny, nz = CELL * n_py, CELL * n_pz
    shape = (n * nf, 128)
    row = lax.broadcasted_iota(jnp.int32, shape, 0)
    col = lax.broadcasted_iota(jnp.int32, shape, 1)

    def square(wave, period):
        folded = jnp.minimum(wave, period - wave).astype(F32)
        return (folded * (2.0 * math.pi / period)) ** 2

    p = row // nf
    wave_x = 2 * (owner * nf + row % nf) + parity
    wave_y = p // n_pz + n_py * (col // CELL % CELL)
    wave_z = p % n_pz + n_pz * (col % CELL)
    total = square(wave_y, ny) + square(wave_z, nz) + square(wave_x, nx)
    safe = jnp.where(total > 0, total, 1.0)
    green = jnp.where(total > 0, -4.0 * math.pi * jnp.exp(-SMOOTHING_SQ * total) / safe, 0.0)
    return green * (jnp.where(wave_x > 0, 1.0, 0.5) * (1.0 / float(ny * nz * nx)))


def kernel(
    n_py, n_pz, nx, nf, chunk,
    pos_hbm, mass_hbm, line_hbm, back_hbm, fwd_hbm, fwd_edge_hbm, inv_hbm, turn_hbm, unturn_hbm,
    pot_ref, side_ref,
    pos_ref, mass_ref, line, back, fwd, fwd_edge, inv, turn, unturn, table_sem,
    acc, green, mixed, send1, recv1, send2, recv2, waves_edge,
    send_sem1, recv_sem1, send_sem2, recv_sem2,
):
    n = n_py * n_pz
    half_nf, half, quarter = nf // 2, nx // 2, nx // 4
    my_y, my_z = lax.axis_index("py"), lax.axis_index("pz")
    rank = my_y * n_pz + my_z

    loads = [
        pltpu.make_async_copy(src, dst, table_sem.at[i])
        for i, (src, dst) in enumerate(
            [
                (pos_hbm, pos_ref),
                (mass_hbm, mass_ref),
                (line_hbm, line),
                (turn_hbm, turn),
                (fwd_hbm, fwd),
                (fwd_edge_hbm, fwd_edge),
                (inv_hbm, inv),
                (unturn_hbm, unturn),
                (back_hbm, back),
            ]
        )
    ]
    for load in loads[:2]:
        load.start()

    n_own, half_z, first_z = n // 2, n_pz // 2, n_pz // 4
    own_z = my_z - first_z
    is_owner = (own_z >= 0) & (own_z < half_z)
    is_guest = jnp.logical_not(is_owner)
    owner = my_y * half_z + own_z
    turn_z = jnp.where(my_z >= half_z, first_z, 0) ^ lax.rem(my_z, 2)

    def far_first(step):
        along = step % n_pz
        return -(along // 4), -bin(step).count("1"), along % 4 // 2, -step

    everyone, readers, owners = [], [], []
    for step in sorted(range(1, n), key=far_first):
        other_y, other_z = (step // n_pz) ^ my_y, (step % n_pz) ^ my_z
        everyone.append((other_y * n_pz + other_z, (other_y, other_z)))
    core = lax.rem(my_z, 2)
    for step in range(n):
        along = step // (2 * n_py)
        other_y, other_z = step // 2 % n_py, 2 * along + ((step % 2) ^ core)
        if along:
            other_y = other_y ^ my_y
        readers.append((2 * along, other_y * n_pz + other_z, (other_y, other_z)))
    for step in sorted(range(n_own), key=lambda v: (-(v % half_z // 2), -bin(v // half_z).count("1"))):
        other_y, other_z = (step // half_z) ^ my_y, (step % half_z) ^ turn_z
        place = (other_y, other_z + first_z)
        owners.append((step < half_z, other_y * half_z + other_z, place))

    barrier = pltpu.get_barrier_semaphore()

    @pl.when(is_owner)
    def _():
        for _, where in everyone:
            pl.semaphore_signal(barrier, inc=1, device_id=where, device_id_type=MESH)

    for load in loads[2:]:
        load.start()
    base_y = (my_y * CELL).astype(F32)
    base_z = (my_z * CELL).astype(F32)
    row_of = lax.broadcasted_iota(jnp.int32, (CELL, chunk), 0)
    cell = row_of.astype(F32)
    sublane = lax.broadcasted_iota(jnp.int32, (2 * CELL, chunk), 0).astype(F32)

    for load in loads[:2]:
        load.wait()

    def deposited(turn_index):
        span = pl.ds(pl.multiple_of(turn_index * chunk, chunk), chunk)
        tall = (CELL, chunk)
        along_y = jnp.broadcast_to(pos_ref[0:1, span], tall) - base_y
        along_z = jnp.broadcast_to(pos_ref[1:2, span], tall) - base_z
        along_x = jnp.broadcast_to(pos_ref[2:3, span], tall)
        mass = jnp.broadcast_to(mass_ref[0:1, span], tall)
        floor_x = jnp.floor(along_x)
        pair = jnp.floor(along_x * 0.5)
        is_even = floor_x == 2.0 * pair
        upper = mass * (along_x - floor_x)
        lower = mass * (1.0 - (along_x - floor_x))
        shares = [
            jnp.where(is_even, lower, 0.0),
            jnp.where(is_even, upper, lower),
            jnp.where(is_even, 0.0, upper),
        ]
        where_x = jnp.concatenate([pair, pair], axis=0).astype(BF16)
        one_hot = jnp.concatenate(
            [
                jnp.where(
                    where_x == (sublane + float(t)).astype(BF16),
                    jnp.ones((), BF16),
                    jnp.zeros((), BF16),
                )
                for t in range(0, half, 2 * CELL)
            ],
            axis=0,
        )
        hat_y = jnp.maximum(1.0 - jnp.abs(along_y - cell), 0.0)
        hat_z = jnp.maximum(1.0 - jnp.abs(along_z - cell), 0.0)
        last_y = jnp.maximum(along_y - (CELL - 1.0), 0.0)
        last_z = jnp.maximum(along_z - (CELL - 1.0), 0.0)
        tiles = []
        for share in shares:
            scaled = hat_z * share
            tiles += [hat_y[a : a + 1] * scaled for a in range(CELL)]
            tiles += [last_y * scaled, hat_y * (last_z * share)]
        corner = jnp.where(row_of == 0, shares[0], jnp.where(row_of == 1, shares[1], shares[2]))
        tiles.append(jnp.where(row_of < 3, corner * (last_y * last_z), 0.0))
        tiles.append(jnp.zeros(tall, F32))
        return split(jnp.concatenate(tiles, axis=0)), one_hot

    turns = pos_ref.shape[1] // chunk

    acc[...] = jnp.zeros_like(acc)

    @pl.loop(0, turns)
    def _(index):
        masses, one_hot = deposited(index)
        for i in range(2):
            acc[i] += dot(masses[i], one_hot, ((1,), (1,)))

    for load in loads[2:3]:
        load.wait()
    sums = acc[0] + acc[1]
    block = CELLS + 2 * CELL
    even = sums[:block] + pltpu.roll(sums[2 * block : 3 * block], 1, 1)
    odd = sums[block : 2 * block]
    corner = sums[3 * block : 3 * block + CELL]
    first = lax.broadcasted_iota(jnp.int32, (CELL, half), 0) == 0
    blank = jnp.zeros((CELL, half), F32)
    corner_even = corner + pltpu.roll(pltpu.roll(corner, CELL - 2, 0), 1, 1)
    corner_even = jnp.where(first, corner_even, 0.0)
    corner_odd = jnp.where(first, pltpu.roll(corner, CELL - 1, 0), 0.0)
    even = jnp.concatenate([even, corner_even, blank], axis=0)
    odd = jnp.concatenate([odd, corner_odd, blank], axis=0)

    lane = lax.broadcasted_iota(jnp.int32, (nf, 128), 1)
    is_real = lane < CELLS
    is_real_edge = lane % CELLS < EDGE
    low_half = lax.broadcasted_iota(jnp.int32, (half_nf, 128), 1) < CELLS
    for parity in range(2):
        folded = []
        for grid in (even, odd):
            left, right = grid[:, :quarter], grid[:, quarter:]
            folded.append(left - right if parity else left + right)
        density = [
            jnp.concatenate([x[:CELLS]] * 2 + [x[CELLS:]] * 4, axis=0)
            for x in split(jnp.concatenate(folded, axis=1))
        ]
        both = dot_parts([line[parity, 0], line[parity, 1]], density, ((1,), (1,)))
        for r in range(n_own):
            re, im = both[r * nf : (r + 1) * nf], both[quarter + r * nf : quarter + (r + 1) * nf]
            send1[parity, r, 0:nf] = jnp.where(is_real, re[:, :128], im[:, :128])
            side = jnp.where(is_real_edge, re[:, 128:], im[:, 128:])
            send1[parity, r, nf : nf + half_nf] = jnp.where(
                low_half, side[:half_nf], side[half_nf:]
            )
        if parity == 0:

            @pl.when(is_owner)
            def _():
                pl.semaphore_wait(barrier, n_own - 1)

            @pl.when(is_guest)
            def _():
                pl.semaphore_wait(barrier, n_own)

        for maybe_self, peer, where in owners:
            copy = pltpu.make_async_remote_copy(
                src_ref=send1.at[parity, peer],
                dst_ref=recv1.at[parity, rank],
                send_sem=send_sem1.at[parity],
                recv_sem=recv_sem1.at[parity],
                device_id=where,
                device_id_type=MESH,
            )
            if maybe_self:
                pl.when(where[1] != my_z)(copy.start)
            else:
                copy.start()

    def wait_for(ref, parity, count, sem):
        span = ref.at[parity, pl.ds(0, count)]
        pltpu.make_async_copy(span, span, sem.at[parity]).wait()

    def every(half_plane, py, pz):
        if pz <= n_pz // 2:
            return half_plane[py, pz], 1
        return half_plane[-py % n_py, n_pz - pz], -1

    def middle(parity):
        turned = []
        for lanes, span, height in (
            (slice(0, 128), slice(0, nf), nf),
            (slice(128, 256), slice(nf, nf + half_nf), half_nf),
        ):
            values = [[recv1[parity, ay * n_pz + az, span] for az in range(n_pz)] for ay in range(n_py)]
            found = plane_forward(values, n_py, n_pz)
            blocks = []
            for p in range(n):
                (re, im), sign = every(found, p // n_pz, p % n_pz)
                c, s = turn[p : p + 1, lanes], turn[n + p : n + p + 1, lanes]
                if im is None:
                    u, v = c * re, -(s * re)
                elif sign > 0:
                    u, v = c * re + s * im, c * im - s * re
                else:
                    u, v = c * re - s * im, -(c * im) - s * re
                blocks.append([u, v])
            turned.append(blocks)
        if parity == 0:
            corner_row = lax.broadcasted_iota(jnp.int32, (half_nf, 128), 0) == 0
            top_row = lax.broadcasted_iota(jnp.int32, (nf, 128), 0) == 0
            level = jnp.sum(turned[0][0][0][0:1] * jnp.where(is_real[0:1], 1.0, 0.0), axis=1, keepdims=True)
            level += jnp.sum(
                turned[1][0][0][0:1] * jnp.where(lane[0:1] < EDGE, 1.0, 0.0), axis=1, keepdims=True
            )
            level = jnp.where(owner == 0, level * (1.0 / CELLS), 0.0)
            flat = turn[2 * n : 2 * n + 1]
            turned[0][0][0] = turned[0][0][0] - jnp.where(top_row, level * flat[:, :128], 0.0)
            turned[1][0][0] = turned[1][0][0] - jnp.where(corner_row, level * flat[:, 128:], 0.0)

        stacked = [
            jnp.concatenate(
                [jnp.concatenate([uv[i] for uv in blocks], axis=0) for i in range(2)], axis=1
            )
            for blocks in turned
        ]
        high, low = split(stacked[0])
        wide = dot(high, fwd[...])
        solved = wide[:, :128] + wide[:, 128:] + dot(low, fwd[:, :128])
        beside = dot_parts(split(stacked[1]), [fwd_edge[0], fwd_edge[1]])
        pieces = []
        for p in range(n):
            rows_of = beside[p * half_nf : (p + 1) * half_nf]
            pieces += [rows_of[:, :128], rows_of[:, 128:]]
        solved = (solved + jnp.concatenate(pieces, axis=0)) * green[parity]
        high, low = split(solved)
        mixed[...] = dot(jnp.concatenate([high, low], axis=1), inv[0:256]) + dot(high, inv[256:384])

        for lanes, offset in ((slice(0, 128), 0), (slice(128, 256), 256)):
            ones, twos = {}, {}
            for p in range(n):
                c, s = unturn[p : p + 1, lanes], unturn[n + p : n + p + 1, lanes]
                span = slice(p * nf, (p + 1) * nf)
                y, jy = mixed[span, offset : offset + 128], mixed[span, offset + 128 : offset + 256]
                ones[p // n_pz, p % n_pz] = c * y + s * jy
                twos[p // n_pz, p % n_pz] = c * jy - s * y
            half_plane = {}
            for pz in range(n_pz // 2 + 1):
                for py in range(n_py):
                    other = (-py % n_py, -pz % n_pz)
                    if other == (py, pz):
                        half_plane[py, pz] = (ones[other] * 2.0, None)
                    else:
                        half_plane[py, pz] = (
                            ones[py, pz] + ones[other],
                            twos[other] - twos[py, pz],
                        )
            values = plane_inverse(half_plane, n_py, n_pz)
            for ay in range(n_py):
                for az in range(n_pz):
                    value = values[ay][az]
                    if offset == 0:
                        send2[parity, ay * n_pz + az, 0:nf] = value
                    else:
                        value = jnp.where(low_half, value[:half_nf], value[half_nf:])
                        send2[parity, ay * n_pz + az, nf : nf + half_nf] = value
        for along, peer, where in readers:
            copy = pltpu.make_async_remote_copy(
                src_ref=send2.at[parity, peer],
                dst_ref=recv2.at[parity, owner],
                send_sem=send_sem2.at[parity],
                recv_sem=recv_sem2.at[parity],
                device_id=where,
                device_id_type=MESH,
            )
            if first_z <= along < first_z + half_z:
                pl.when(peer != rank)(copy.start)
            else:
                copy.start()
        recv2[parity, owner] = send2[parity, rank]

    @pl.when(is_owner)
    def _():
        for parity in range(2):
            recv1[parity, rank] = send1[parity, owner]
            green[parity] = green_factor(owner, parity, n_py, n_pz, nx, nf)
        for load in loads[3:8]:
            load.wait()
        for parity in range(2):
            with jax.named_scope("wait1"):
                wait_for(recv1, parity, n - 1, recv_sem1)
            with jax.named_scope("mid"):
                middle(parity)

    @pl.when(is_guest)
    def _():
        for load in loads[3:8]:
            load.wait()

    loads[8].wait()
    found = []
    for parity in range(2):
        with jax.named_scope("wait2"):

            @pl.when(is_owner)
            def _():
                wait_for(recv2, parity, n_own - 1, recv_sem2)

            @pl.when(is_guest)
            def _():
                wait_for(recv2, parity, n_own, recv_sem2)

        for r in range(n_own):
            waves_edge[r * half_nf : (r + 1) * half_nf] = recv2[parity, r, nf : nf + half_nf]
        beside = jnp.transpose(waves_edge[...])
        rows_of = [
            recv2[parity, r, h * half_nf : (h + 1) * half_nf]
            for h in range(2)
            for r in range(n_own)
        ]
        inner = jnp.transpose(jnp.concatenate(rows_of, axis=0))
        columns = []
        for c in range(2):
            pieces = [
                beside[h * CELLS + c * EDGE : h * CELLS + (c + 1) * EDGE] for h in range(2)
            ]
            columns.append(
                jnp.concatenate(
                    [inner[c * CELLS : (c + 1) * CELLS], jnp.concatenate(pieces, axis=1)], axis=0
                )
            )
        found.append(
            dot_parts(
                split(jnp.concatenate(columns, axis=1), 3), [back[parity, i] for i in range(3)]
            )
        )
    for side, value in enumerate((found[0] + found[1], found[0] - found[1])):
        span = slice(side * half, (side + 1) * half)
        for a in range(CELL):
            pot_ref[a, :, span] = value[a * CELL : (a + 1) * CELL]
        for i in range(4):
            side_ref[i, :, span] = value[CELLS + i * CELL : CELLS + (i + 1) * CELL]

    @pl.when(is_owner)
    def _():
        for parity in range(2):
            wait_for(send1, parity, n_own - 1, send_sem1)
            wait_for(send2, parity, n - 1, send_sem2)

    @pl.when(is_guest)
    def _():
        for parity in range(2):
            wait_for(send1, parity, n_own, send_sem1)


def finish(pot_ref, side_ref, out_hbm, out_ref, sems):
    nx = pot_ref.shape[2]
    copies = []

    def emit(d):
        copies.append(pltpu.make_async_copy(out_ref.at[d], out_hbm.at[d], sems.at[d]))
        copies[-1].start()

    for a in range(CELL):
        tile = pot_ref[a]
        out_ref[2, a] = (pltpu.roll(tile, 1, 1) - pltpu.roll(tile, nx - 1, 1)) * 0.5
    emit(2)
    for a in range(CELL):
        below = pot_ref[a - 1] if a else side_ref[0]
        above = pot_ref[a + 1] if a < CELL - 1 else side_ref[1]
        out_ref[0, a] = (below - above) * 0.5
    emit(0)
    before, after = side_ref[2], side_ref[3]
    lane_row = lax.broadcasted_iota(jnp.int32, (CELL, nx), 0)
    for a in range(CELL):
        tile = pot_ref[a]
        lower = jnp.where(lane_row == 0, before[a : a + 1], pltpu.roll(tile, 1, 0))
        upper = jnp.where(lane_row == CELL - 1, after[a : a + 1], pltpu.roll(tile, CELL - 1, 0))
        out_ref[1, a] = (lower - upper) * 0.5
    emit(1)
    for copy in copies:
        copy.wait()


def solution(mesh):
    n_py, n_pz = mesh.shape["py"], mesh.shape["pz"]
    n = n_py * n_pz
    nx = 512
    nf = nx // 4 // (n // 2)
    consts = tables(n_py, n_pz, nx, nf)

    def shards(positions, masses):
        chunk = min(positions.shape[1], 2048)
        vmem = pl.BlockSpec(memory_space=pltpu.VMEM)
        hbm = pl.BlockSpec(memory_space=pltpu.HBM)
        dma = pltpu.SemaphoreType.DMA
        rows = nf + nf // 2
        few, all_of = (pltpu.VMEM((2, count, rows, 128), F32) for count in (n // 2, n))
        operands = [positions, masses.reshape(1, -1), *map(jnp.asarray, consts)]
        pot, side = pl.pallas_call(
            functools.partial(kernel, n_py, n_pz, nx, nf, chunk),
            out_shape=[pltpu.VMEM((CELL, CELL, nx), F32), pltpu.VMEM((4, CELL, nx), F32)],
            in_specs=[hbm] * len(operands),
            out_specs=[vmem, vmem],
            scratch_shapes=[
                *[pltpu.VMEM(x.shape, x.dtype) for x in operands],
                dma((len(operands),)),
                pltpu.VMEM((2, 3 * (CELLS + 2 * CELL) + 2 * CELL, nx // 2), F32),
                pltpu.VMEM((2, n * nf, 128), F32),
                pltpu.VMEM((n * nf, 512), F32),
                few, all_of, all_of, few,
                pltpu.VMEM((n // 2 * (nf // 2), 128), F32),
                dma((2,)), dma((2,)), dma((2,)), dma((2,)),
            ],
            compiler_params=pltpu.CompilerParams(
                collective_id=0, has_side_effects=True, vmem_limit_bytes=50 << 20
            ),
        )(*[pltpu.with_memory_space_constraint(x, pltpu.HBM) for x in operands])
        return pl.pallas_call(
            finish,
            out_shape=jax.ShapeDtypeStruct((3, CELL, CELL, nx), F32),
            in_specs=[vmem, vmem],
            out_specs=hbm,
            scratch_shapes=[pltpu.VMEM((3, CELL, CELL, nx), F32), dma((3,))],
            compiler_params=pltpu.CompilerParams(vmem_limit_bytes=16 << 20),
        )(pot, side)

    return jax.shard_map(
        shards,
        mesh=mesh,
        in_specs=(P(None, ("py", "pz")), P(("py", "pz"))),
        out_specs=P(None, "py", "pz", None),
        check_vma=False,
    )
```

```python
import functools
import math

import jax
import jax.numpy as jnp
import ml_dtypes
import numpy as np
from jax import lax
from jax.experimental import pallas as pl
from jax.experimental.pallas import tpu as pltpu
from jax.sharding import PartitionSpec as P

MESH = pl.DeviceIdType.MESH
F32 = jnp.float32
BF16 = jnp.bfloat16
SMOOTHING_SQ = 0.25
CELL = 8
CELLS = CELL * CELL
EDGE = 32


def parts(table, count):
    out = []
    for _ in range(count):
        out.append(table.astype(ml_dtypes.bfloat16))
        table = table - out[-1].astype(np.float64)
    return np.stack(out)


def real_form(wave, turned):
    wave = wave * 1j if turned else wave
    return np.block([[wave.real, wave.imag], [-wave.imag, wave.real]])


def tables(n_py, n_pz, nx, nf):
    n = n_py * n_pz
    ny, nz = CELL * n_py, CELL * n_pz
    quarter, half_nf = nx // 4, nf // 2
    along = (2 * np.arange(quarter)[None, :] + np.arange(2)[:, None]).reshape(-1)
    order = np.arange(quarter).reshape(n // 2, 2, half_nf).transpose(1, 0, 2).reshape(-1)
    line, back = [], []
    for odd in range(2):
        waves = 2 * np.arange(quarter) + odd
        phase = (np.outer(waves, along) % nx) * (2 * np.pi / nx)
        line.append(parts(np.concatenate([np.cos(phase), -np.sin(phase)]), 2))
        phase = (np.outer(waves[order], np.arange(nx // 2)) % nx) * (2 * np.pi / nx)
        back.append(parts(np.concatenate([np.cos(phase), -np.sin(phase)]), 3))

    inner = [(a, z) for a in range(CELL) for z in range(CELL)]
    upper = [(CELL, z) for z in range(CELL)] + [(a, CELL) for a in range(CELL)] + [(CELL, CELL)]
    outer = [(-1, z) for z in range(CELL)] + [(CELL, z) for z in range(CELL)]
    outer += [(a, -1) for a in range(CELL)] + [(a, CELL) for a in range(CELL)]
    used = np.zeros(EDGE)
    used[: len(upper)] = 1.0
    upper = np.array(upper + [(0, 0)] * (EDGE - len(upper)))
    inner, outer = np.array(inner), np.array(outer)

    def inside(cells, sign):
        return np.exp(sign * 2j * np.pi * (cells @ np.array(inner).T) / CELL)

    def twiddles(cells, copies):
        p = np.arange(n)
        phase = 2 * np.pi * (
            np.outer(p // n_pz, cells[:, 0]) / ny + np.outer(p % n_pz, cells[:, 1]) / nz
        )
        return np.tile(np.stack([np.cos(phase), np.sin(phase)]), (1, 1, copies))

    share = lambda at: np.where((at == 0) | (at == CELL), 0.5, 1.0)
    flat = share(inner[:, 0]) * share(inner[:, 1])
    flat_edge = share(upper[:, 0]) * share(upper[:, 1]) * used
    pattern = np.zeros((CELL, 256))
    pattern[0, :CELLS] = flat
    pattern[0, 128 : 128 + EDGE] = flat_edge
    turn = np.concatenate([twiddles(inner, 2), twiddles(upper, 4)], axis=2).reshape(2 * n, 256)
    turn = np.concatenate([turn, pattern]).astype(np.float32)
    unturn = np.concatenate([twiddles(inner, 2), twiddles(outer, 4)], axis=2)
    unturn = unturn.reshape(2 * n, 256).astype(np.float32)

    wave = inside(inner, -1)
    fwd = parts(np.concatenate([real_form(wave, 0), real_form(wave, 1)]), 2)
    fwd = np.concatenate([fwd[0], fwd[1]], axis=1)
    wave = inside(upper, -1) * used[:, None]
    spread = [np.kron(np.eye(2), real_form(wave, t)) for t in range(2)]
    fwd_edge = parts(np.concatenate(spread), 2)
    wave, wave_edge = inside(inner, 1).T, inside(outer, 1).T
    pieces = [real_form(wave, 0), real_form(wave, 1)]
    pieces += [np.tile(real_form(wave_edge, t), (1, 2)) for t in range(2)]
    inv = parts(np.concatenate(pieces, axis=1), 2)
    inv = np.concatenate([inv[0], inv[0], inv[1]])
    return np.stack(line), np.stack(back), fwd, fwd_edge, inv, turn, unturn


def plus(a, b):
    return b if a is None else a if b is None else a + b


def minus(a, b):
    return a if b is None else -b if a is None else a - b


def conj(x):
    return x[0], minus(None, x[1]) if x[1] is not None else None


def add(x, y):
    return plus(x[0], y[0]), plus(x[1], y[1])


def sub(x, y):
    return minus(x[0], y[0]), minus(x[1], y[1])


def rotated(x, k, n, sign):
    re, im = x
    if k == 0:
        return x
    if 4 * k == n:
        turned = (minus(None, im) if im is not None else None, re)
        return turned if sign > 0 else (im, -re)
    c, s = math.cos(2 * math.pi * k / n), sign * math.sin(2 * math.pi * k / n)
    if im is None:
        return re * c, re * s
    if 8 * k == n:
        both = (re - im, re + im) if sign > 0 else (re + im, im - re)
        return both[0] * c, both[1] * c
    return re * c - im * s, re * s + im * c


def fft(x, sign):
    n = len(x)
    if n == 1:
        return x
    even, odd = fft(x[::2], sign), fft(x[1::2], sign)
    odd = [rotated(o, k, n, sign) for k, o in enumerate(odd)]
    return [add(e, o) for e, o in zip(even, odd)] + [sub(e, o) for e, o in zip(even, odd)]


def rfft(x):
    n = len(x)
    if n == 1:
        return [(x[0], None)]
    if n == 2:
        return [(x[0] + x[1], None), (x[0] - x[1], None)]
    even, odd = rfft(x[::2]), rfft(x[1::2])
    out = [None] * (n // 2 + 1)
    for k in range(n // 4 + 1):
        turned = rotated(odd[k], k, n, -1)
        out[k] = add(even[k], turned)
        if k < n // 4:
            out[n // 2 - k] = conj(sub(even[k], turned))
    return out


def irfft(x):
    n = 2 * (len(x) - 1)
    if n == 2:
        return [x[0][0] + x[1][0], x[0][0] - x[1][0]]
    even, odd = [], []
    for k in range(n // 4 + 1):
        if 4 * k == n:
            even.append((x[k][0] * 2.0, None))
            odd.append((x[k][1] * -2.0, None) if x[k][1] is not None else (x[k][0] * 0.0, None))
            continue
        mirror = conj(x[n // 2 - k])
        even.append(add(x[k], mirror))
        odd.append(rotated(sub(x[k], mirror), k, n, 1))
    even, odd = irfft(even), irfft(odd)
    return [v for pair in zip(even, odd) for v in pair]


def plane_forward(values, n_py, n_pz):
    lines = [rfft(row) for row in values]
    out = {}
    for pz in range(n_pz // 2 + 1):
        column = [line[pz] for line in lines]
        if all(x[1] is None for x in column):
            found = rfft([x[0] for x in column])
            found += [conj(found[n_py - py]) for py in range(n_py // 2 + 1, n_py)]
        else:
            found = fft(column, -1)
        for py in range(n_py):
            out[py, pz] = found[py]
    return out


def plane_inverse(half, n_py, n_pz):
    columns = []
    for pz in range(n_pz // 2 + 1):
        if pz in (0, n_pz // 2):
            column = irfft([half[py, pz] for py in range(n_py // 2 + 1)])
            columns.append([(x, None) for x in column])
        else:
            columns.append(fft([half[py, pz] for py in range(n_py)], 1))
    return [irfft([column[ay] for column in columns]) for ay in range(n_py)]


def split(x, count=2):
    out = []
    for i in range(count):
        out.append(x.astype(BF16))
        if i < count - 1:
            x = x - out[-1].astype(F32)
    return out


def dot(left, right, dims=((1,), (0,))):
    return lax.dot_general(left, right, (dims, ((), ())), preferred_element_type=F32)


def dot_parts(left, right, dims=((1,), (0,))):
    count = len(left)
    total = None
    for order in reversed(range(count)):
        for i in range(order + 1):
            term = dot(left[i], right[order - i], dims)
            total = term if total is None else total + term
    return total


def green_factor(owner, parity, n_py, n_pz, nx, nf):
    n = n_py * n_pz
    ny, nz = CELL * n_py, CELL * n_pz
    shape = (n * nf, 128)
    row = lax.broadcasted_iota(jnp.int32, shape, 0)
    col = lax.broadcasted_iota(jnp.int32, shape, 1)

    def square(wave, period):
        folded = jnp.minimum(wave, period - wave).astype(F32)
        return (folded * (2.0 * math.pi / period)) ** 2

    p = row // nf
    wave_x = 2 * (owner * nf + row % nf) + parity
    wave_y = p // n_pz + n_py * (col // CELL % CELL)
    wave_z = p % n_pz + n_pz * (col % CELL)
    total = square(wave_y, ny) + square(wave_z, nz) + square(wave_x, nx)
    safe = jnp.where(total > 0, total, 1.0)
    green = jnp.where(total > 0, -4.0 * math.pi * jnp.exp(-SMOOTHING_SQ * total) / safe, 0.0)
    return green * (jnp.where(wave_x > 0, 1.0, 0.5) * (1.0 / float(ny * nz * nx)))


def kernel(
    n_py, n_pz, nx, nf, chunk,
    pos_hbm, mass_hbm, line_hbm, back_hbm, fwd_hbm, fwd_edge_hbm, inv_hbm, turn_hbm, unturn_hbm,
    pot_ref, side_ref,
    pos_ref, mass_ref, line, back, fwd, fwd_edge, inv, turn, unturn, table_sem,
    piece_sem, acc, green, mixed, send1, recv1, send2, recv2, waves_edge,
    send_sem1, recv_sem1, send_sem2, recv_sem2,
):
    n = n_py * n_pz
    half_nf, half, quarter = nf // 2, nx // 2, nx // 4
    my_y, my_z = lax.axis_index("py"), lax.axis_index("pz")
    rank = my_y * n_pz + my_z

    loads = [
        pltpu.make_async_copy(src, dst, table_sem.at[i])
        for i, (src, dst) in enumerate(
            [
                (line_hbm, line),
                (turn_hbm, turn),
                (fwd_hbm, fwd),
                (fwd_edge_hbm, fwd_edge),
                (inv_hbm, inv),
                (unturn_hbm, unturn),
                (back_hbm, back),
            ]
        )
    ]
    pieces = []
    width = pos_ref.shape[1] // 2
    for i in range(2):
        span = pl.ds(i * width, width)
        for src, dst in ((pos_hbm, pos_ref), (mass_hbm, mass_ref)):
            pieces.append(
                pltpu.make_async_copy(src.at[:, span], dst.at[:, span], piece_sem.at[len(pieces)])
            )
            pieces[-1].start()

    n_own, half_z, first_z = n // 2, n_pz // 2, n_pz // 4
    own_z = my_z - first_z
    is_owner = (own_z >= 0) & (own_z < half_z)
    is_guest = jnp.logical_not(is_owner)
    owner = my_y * half_z + own_z
    turn_z = jnp.where(my_z >= half_z, first_z, 0) ^ lax.rem(my_z, 2)

    def far_first(step):
        along = step % n_pz
        return -(along // 4), -bin(step).count("1"), along % 4 // 2, -step

    everyone, readers, owners = [], [], []
    for step in sorted(range(1, n), key=far_first):
        other_y, other_z = (step // n_pz) ^ my_y, (step % n_pz) ^ my_z
        everyone.append((other_y * n_pz + other_z, (other_y, other_z)))
    core = lax.rem(my_z, 2)
    for step in range(n):
        along = step // (2 * n_py)
        other_y, other_z = step // 2 % n_py, 2 * along + step % 2
        if along:
            other_y, other_z = other_y ^ my_y, other_z ^ core
        readers.append((2 * along, other_y * n_pz + other_z, (other_y, other_z)))
    for step in sorted(range(n_own), key=lambda v: (-(v % half_z // 2), -bin(v // half_z).count("1"))):
        other_y, other_z = (step // half_z) ^ my_y, (step % half_z) ^ turn_z
        place = (other_y, other_z + first_z)
        owners.append((step < half_z, other_y * half_z + other_z, place))

    barrier = pltpu.get_barrier_semaphore()

    @pl.when(is_owner)
    def _():
        for _, where in everyone:
            pl.semaphore_signal(barrier, inc=1, device_id=where, device_id_type=MESH)

    for load in loads:
        load.start()
    base_y = (my_y * CELL).astype(F32)
    base_z = (my_z * CELL).astype(F32)
    row_of = lax.broadcasted_iota(jnp.int32, (CELL, chunk), 0)
    cell = row_of.astype(F32)
    sublane = lax.broadcasted_iota(jnp.int32, (2 * CELL, chunk), 0).astype(F32)

    for load in pieces:
        load.wait()

    def deposited(turn_index):
        span = pl.ds(pl.multiple_of(turn_index * chunk, chunk), chunk)
        tall = (CELL, chunk)
        along_y = jnp.broadcast_to(pos_ref[0:1, span], tall) - base_y
        along_z = jnp.broadcast_to(pos_ref[1:2, span], tall) - base_z
        along_x = jnp.broadcast_to(pos_ref[2:3, span], tall)
        mass = jnp.broadcast_to(mass_ref[0:1, span], tall)
        floor_x = jnp.floor(along_x)
        pair = jnp.floor(along_x * 0.5)
        is_even = floor_x == 2.0 * pair
        upper = mass * (along_x - floor_x)
        lower = mass * (1.0 - (along_x - floor_x))
        shares = [
            jnp.where(is_even, lower, 0.0),
            jnp.where(is_even, upper, lower),
            jnp.where(is_even, 0.0, upper),
        ]
        where_x = jnp.concatenate([pair, pair], axis=0).astype(BF16)
        one_hot = jnp.concatenate(
            [
                jnp.where(
                    where_x == (sublane + float(t)).astype(BF16),
                    jnp.ones((), BF16),
                    jnp.zeros((), BF16),
                )
                for t in range(0, half, 2 * CELL)
            ],
            axis=0,
        )
        hat_y = jnp.maximum(1.0 - jnp.abs(along_y - cell), 0.0)
        hat_z = jnp.maximum(1.0 - jnp.abs(along_z - cell), 0.0)
        last_y = jnp.maximum(along_y - (CELL - 1.0), 0.0)
        last_z = jnp.maximum(along_z - (CELL - 1.0), 0.0)
        tiles = []
        for share in shares:
            scaled = hat_z * share
            tiles += [hat_y[a : a + 1] * scaled for a in range(CELL)]
            tiles += [last_y * scaled, hat_y * (last_z * share)]
        corner = jnp.where(row_of == 0, shares[0], jnp.where(row_of == 1, shares[1], shares[2]))
        tiles.append(jnp.where(row_of < 3, corner * (last_y * last_z), 0.0))
        tiles.append(jnp.zeros(tall, F32))
        return split(jnp.concatenate(tiles, axis=0)), one_hot

    turns = pos_ref.shape[1] // chunk

    acc[...] = jnp.zeros_like(acc)

    @pl.loop(0, turns)
    def _(index):
        masses, one_hot = deposited(index)
        for i in range(2):
            acc[i] += dot(masses[i], one_hot, ((1,), (1,)))

    for load in loads[:1]:
        load.wait()
    sums = acc[0] + acc[1]
    block = CELLS + 2 * CELL
    even = sums[:block] + pltpu.roll(sums[2 * block : 3 * block], 1, 1)
    odd = sums[block : 2 * block]
    corner = sums[3 * block : 3 * block + CELL]
    first = lax.broadcasted_iota(jnp.int32, (CELL, half), 0) == 0
    blank = jnp.zeros((CELL, half), F32)
    corner_even = corner + pltpu.roll(pltpu.roll(corner, CELL - 2, 0), 1, 1)
    corner_even = jnp.where(first, corner_even, 0.0)
    corner_odd = jnp.where(first, pltpu.roll(corner, CELL - 1, 0), 0.0)
    even = jnp.concatenate([even, corner_even, blank], axis=0)
    odd = jnp.concatenate([odd, corner_odd, blank], axis=0)

    lane = lax.broadcasted_iota(jnp.int32, (nf, 128), 1)
    is_real = lane < CELLS
    is_real_edge = lane % CELLS < EDGE
    low_half = lax.broadcasted_iota(jnp.int32, (half_nf, 128), 1) < CELLS
    for parity in range(2):
        folded = []
        for grid in (even, odd):
            left, right = grid[:, :quarter], grid[:, quarter:]
            folded.append(left - right if parity else left + right)
        density = [
            jnp.concatenate([x[:CELLS]] * 2 + [x[CELLS:]] * 4, axis=0)
            for x in split(jnp.concatenate(folded, axis=1))
        ]
        both = dot_parts([line[parity, 0], line[parity, 1]], density, ((1,), (1,)))
        for r in range(n_own):
            re, im = both[r * nf : (r + 1) * nf], both[quarter + r * nf : quarter + (r + 1) * nf]
            send1[parity, r, 0:nf] = jnp.where(is_real, re[:, :128], im[:, :128])
            side = jnp.where(is_real_edge, re[:, 128:], im[:, 128:])
            send1[parity, r, nf : nf + half_nf] = jnp.where(
                low_half, side[:half_nf], side[half_nf:]
            )
        if parity == 0:

            @pl.when(is_owner)
            def _():
                pl.semaphore_wait(barrier, n_own - 1)

            @pl.when(is_guest)
            def _():
                pl.semaphore_wait(barrier, n_own)

        for maybe_self, peer, where in owners:
            copy = pltpu.make_async_remote_copy(
                src_ref=send1.at[parity, peer],
                dst_ref=recv1.at[parity, rank],
                send_sem=send_sem1.at[parity],
                recv_sem=recv_sem1.at[parity],
                device_id=where,
                device_id_type=MESH,
            )
            if maybe_self:
                pl.when(where[1] != my_z)(copy.start)
            else:
                copy.start()

    def wait_for(ref, parity, count, sem):
        span = ref.at[parity, pl.ds(0, count)]
        pltpu.make_async_copy(span, span, sem.at[parity]).wait()

    def every(half_plane, py, pz):
        if pz <= n_pz // 2:
            return half_plane[py, pz], 1
        return half_plane[-py % n_py, n_pz - pz], -1

    def middle(parity):
        turned = []
        for lanes, span, height in (
            (slice(0, 128), slice(0, nf), nf),
            (slice(128, 256), slice(nf, nf + half_nf), half_nf),
        ):
            values = [[recv1[parity, ay * n_pz + az, span] for az in range(n_pz)] for ay in range(n_py)]
            found = plane_forward(values, n_py, n_pz)
            blocks = []
            for p in range(n):
                (re, im), sign = every(found, p // n_pz, p % n_pz)
                c, s = turn[p : p + 1, lanes], turn[n + p : n + p + 1, lanes]
                if im is None:
                    u, v = c * re, -(s * re)
                elif sign > 0:
                    u, v = c * re + s * im, c * im - s * re
                else:
                    u, v = c * re - s * im, -(c * im) - s * re
                blocks.append([u, v])
            turned.append(blocks)
        if parity == 0:
            corner_row = lax.broadcasted_iota(jnp.int32, (half_nf, 128), 0) == 0
            top_row = lax.broadcasted_iota(jnp.int32, (nf, 128), 0) == 0
            level = jnp.sum(turned[0][0][0][0:1] * jnp.where(is_real[0:1], 1.0, 0.0), axis=1, keepdims=True)
            level += jnp.sum(
                turned[1][0][0][0:1] * jnp.where(lane[0:1] < EDGE, 1.0, 0.0), axis=1, keepdims=True
            )
            level = jnp.where(owner == 0, level * (1.0 / CELLS), 0.0)
            flat = turn[2 * n : 2 * n + 1]
            turned[0][0][0] = turned[0][0][0] - jnp.where(top_row, level * flat[:, :128], 0.0)
            turned[1][0][0] = turned[1][0][0] - jnp.where(corner_row, level * flat[:, 128:], 0.0)

        stacked = [
            jnp.concatenate(
                [jnp.concatenate([uv[i] for uv in blocks], axis=0) for i in range(2)], axis=1
            )
            for blocks in turned
        ]
        high, low = split(stacked[0])
        wide = dot(high, fwd[...])
        solved = wide[:, :128] + wide[:, 128:] + dot(low, fwd[:, :128])
        beside = dot_parts(split(stacked[1]), [fwd_edge[0], fwd_edge[1]])
        pieces = []
        for p in range(n):
            rows_of = beside[p * half_nf : (p + 1) * half_nf]
            pieces += [rows_of[:, :128], rows_of[:, 128:]]
        solved = (solved + jnp.concatenate(pieces, axis=0)) * green[parity]
        high, low = split(solved)
        mixed[...] = dot(jnp.concatenate([high, low], axis=1), inv[0:256]) + dot(high, inv[256:384])

        for lanes, offset in ((slice(0, 128), 0), (slice(128, 256), 256)):
            ones, twos = {}, {}
            for p in range(n):
                c, s = unturn[p : p + 1, lanes], unturn[n + p : n + p + 1, lanes]
                span = slice(p * nf, (p + 1) * nf)
                y, jy = mixed[span, offset : offset + 128], mixed[span, offset + 128 : offset + 256]
                ones[p // n_pz, p % n_pz] = c * y + s * jy
                twos[p // n_pz, p % n_pz] = c * jy - s * y
            half_plane = {}
            for pz in range(n_pz // 2 + 1):
                for py in range(n_py):
                    other = (-py % n_py, -pz % n_pz)
                    if other == (py, pz):
                        half_plane[py, pz] = (ones[other] * 2.0, None)
                    else:
                        half_plane[py, pz] = (
                            ones[py, pz] + ones[other],
                            twos[other] - twos[py, pz],
                        )
            values = plane_inverse(half_plane, n_py, n_pz)
            for ay in range(n_py):
                for az in range(n_pz):
                    value = values[ay][az]
                    if offset == 0:
                        send2[parity, ay * n_pz + az, 0:nf] = value
                    else:
                        value = jnp.where(low_half, value[:half_nf], value[half_nf:])
                        send2[parity, ay * n_pz + az, nf : nf + half_nf] = value
        def deliver(which, chosen):
            for along, peer, where in readers:
                if along not in chosen:
                    continue
                copy = pltpu.make_async_remote_copy(
                    src_ref=send2.at[which, peer],
                    dst_ref=recv2.at[which, owner],
                    send_sem=send_sem2.at[which],
                    recv_sem=recv_sem2.at[which],
                    device_id=where,
                    device_id_type=MESH,
                )
                if first_z <= along < first_z + half_z:
                    pl.when(peer != rank)(copy.start)
                else:
                    copy.start()

        planes = list(range(0, n_pz, 2))
        near, far = planes[:1], planes[-1:]
        inner = planes[1:-1]
        half_in = len(inner) // 2
        if parity == 0:
            deliver(0, near + far)
        else:
            deliver(1, near + far)
            for along in inner:
                deliver(0, [along])
                deliver(1, [along])
        recv2[parity, owner] = send2[parity, rank]

    @pl.when(is_owner)
    def _():
        for parity in range(2):
            recv1[parity, rank] = send1[parity, owner]
            green[parity] = green_factor(owner, parity, n_py, n_pz, nx, nf)
        for load in loads[1:6]:
            load.wait()
        for parity in range(2):
            with jax.named_scope("wait1"):
                wait_for(recv1, parity, n - 1, recv_sem1)
            with jax.named_scope("mid"):
                middle(parity)

    @pl.when(is_guest)
    def _():
        for load in loads[1:6]:
            load.wait()

    loads[6].wait()
    found = []
    for parity in range(2):
        with jax.named_scope("wait2"):

            @pl.when(is_owner)
            def _():
                wait_for(recv2, parity, n_own - 1, recv_sem2)

            @pl.when(is_guest)
            def _():
                wait_for(recv2, parity, n_own, recv_sem2)

        for r in range(n_own):
            waves_edge[r * half_nf : (r + 1) * half_nf] = recv2[parity, r, nf : nf + half_nf]
        beside = jnp.transpose(waves_edge[...])
        rows_of = [
            recv2[parity, r, h * half_nf : (h + 1) * half_nf]
            for h in range(2)
            for r in range(n_own)
        ]
        inner = jnp.transpose(jnp.concatenate(rows_of, axis=0))
        columns = []
        for c in range(2):
            pieces = [
                beside[h * CELLS + c * EDGE : h * CELLS + (c + 1) * EDGE] for h in range(2)
            ]
            columns.append(
                jnp.concatenate(
                    [inner[c * CELLS : (c + 1) * CELLS], jnp.concatenate(pieces, axis=1)], axis=0
                )
            )
        found.append(
            dot_parts(
                split(jnp.concatenate(columns, axis=1), 3), [back[parity, i] for i in range(3)]
            )
        )
    for side, value in enumerate((found[0] + found[1], found[0] - found[1])):
        span = slice(side * half, (side + 1) * half)
        for a in range(CELL):
            pot_ref[a, :, span] = value[a * CELL : (a + 1) * CELL]
        for i in range(4):
            side_ref[i, :, span] = value[CELLS + i * CELL : CELLS + (i + 1) * CELL]

    @pl.when(is_owner)
    def _():
        for parity in range(2):
            wait_for(send1, parity, n_own - 1, send_sem1)
            wait_for(send2, parity, n - 1, send_sem2)

    @pl.when(is_guest)
    def _():
        for parity in range(2):
            wait_for(send1, parity, n_own, send_sem1)


def finish(pot_ref, side_ref, out_hbm, out_ref, sems):
    nx = pot_ref.shape[2]
    copies = []

    def emit(d):
        copies.append(pltpu.make_async_copy(out_ref.at[d], out_hbm.at[d], sems.at[d]))
        copies[-1].start()

    for a in range(CELL):
        tile = pot_ref[a]
        out_ref[2, a] = (pltpu.roll(tile, 1, 1) - pltpu.roll(tile, nx - 1, 1)) * 0.5
    emit(2)
    for a in range(CELL):
        below = pot_ref[a - 1] if a else side_ref[0]
        above = pot_ref[a + 1] if a < CELL - 1 else side_ref[1]
        out_ref[0, a] = (below - above) * 0.5
    emit(0)
    before, after = side_ref[2], side_ref[3]
    lane_row = lax.broadcasted_iota(jnp.int32, (CELL, nx), 0)
    for a in range(CELL):
        tile = pot_ref[a]
        lower = jnp.where(lane_row == 0, before[a : a + 1], pltpu.roll(tile, 1, 0))
        upper = jnp.where(lane_row == CELL - 1, after[a : a + 1], pltpu.roll(tile, CELL - 1, 0))
        out_ref[1, a] = (lower - upper) * 0.5
    emit(1)
    for copy in copies:
        copy.wait()


def solution(mesh):
    n_py, n_pz = mesh.shape["py"], mesh.shape["pz"]
    n = n_py * n_pz
    nx = 512
    nf = nx // 4 // (n // 2)
    consts = tables(n_py, n_pz, nx, nf)

    def shards(positions, masses):
        chunk = min(positions.shape[1], 2048)
        vmem = pl.BlockSpec(memory_space=pltpu.VMEM)
        hbm = pl.BlockSpec(memory_space=pltpu.HBM)
        dma = pltpu.SemaphoreType.DMA
        rows = nf + nf // 2
        few, all_of = (pltpu.VMEM((2, count, rows, 128), F32) for count in (n // 2, n))
        operands = [positions, masses.reshape(1, -1), *map(jnp.asarray, consts)]
        pot, side = pl.pallas_call(
            functools.partial(kernel, n_py, n_pz, nx, nf, chunk),
            out_shape=[pltpu.VMEM((CELL, CELL, nx), F32), pltpu.VMEM((4, CELL, nx), F32)],
            in_specs=[hbm] * len(operands),
            out_specs=[vmem, vmem],
            scratch_shapes=[
                *[pltpu.VMEM(x.shape, x.dtype) for x in operands],
                dma((len(operands),)),
                dma((4,)),
                pltpu.VMEM((2, 3 * (CELLS + 2 * CELL) + 2 * CELL, nx // 2), F32),
                pltpu.VMEM((2, n * nf, 128), F32),
                pltpu.VMEM((n * nf, 512), F32),
                few, all_of, all_of, few,
                pltpu.VMEM((n // 2 * (nf // 2), 128), F32),
                dma((2,)), dma((2,)), dma((2,)), dma((2,)),
            ],
            compiler_params=pltpu.CompilerParams(
                collective_id=0, has_side_effects=True, vmem_limit_bytes=50 << 20
            ),
        )(*[pltpu.with_memory_space_constraint(x, pltpu.HBM) for x in operands])
        return pl.pallas_call(
            finish,
            out_shape=jax.ShapeDtypeStruct((3, CELL, CELL, nx), F32),
            in_specs=[vmem, vmem],
            out_specs=hbm,
            scratch_shapes=[pltpu.VMEM((3, CELL, CELL, nx), F32), dma((3,))],
            compiler_params=pltpu.CompilerParams(vmem_limit_bytes=16 << 20),
        )(pot, side)

    return jax.shard_map(
        shards,
        mesh=mesh,
        in_specs=(P(None, ("py", "pz")), P(("py", "pz"))),
        out_specs=P(None, "py", "pz", None),
        check_vma=False,
    )
```

```python
import functools
import math

import jax
import jax.numpy as jnp
import ml_dtypes
import numpy as np
from jax import lax
from jax.experimental import pallas as pl
from jax.experimental.pallas import tpu as pltpu
from jax.sharding import PartitionSpec as P

MESH = pl.DeviceIdType.MESH
F32 = jnp.float32
BF16 = jnp.bfloat16
SMOOTHING_SQ = 0.25
CELL = 8
CELLS = CELL * CELL
EDGE = 32


def parts(table, count):
    out = []
    for _ in range(count):
        out.append(table.astype(ml_dtypes.bfloat16))
        table = table - out[-1].astype(np.float64)
    return np.stack(out)


def real_form(wave, turned):
    wave = wave * 1j if turned else wave
    return np.block([[wave.real, wave.imag], [-wave.imag, wave.real]])


def tables(n_py, n_pz, nx, nf):
    n = n_py * n_pz
    ny, nz = CELL * n_py, CELL * n_pz
    quarter, half_nf = nx // 4, nf // 2
    along = (2 * np.arange(quarter)[None, :] + np.arange(2)[:, None]).reshape(-1)
    order = np.arange(quarter).reshape(n // 2, 2, half_nf).transpose(1, 0, 2).reshape(-1)
    line, back = [], []
    for odd in range(2):
        waves = 2 * np.arange(quarter) + odd
        phase = (np.outer(waves, along) % nx) * (2 * np.pi / nx)
        line.append(parts(np.concatenate([np.cos(phase), -np.sin(phase)]), 2))
        phase = (np.outer(waves[order], np.arange(nx // 2)) % nx) * (2 * np.pi / nx)
        back.append(parts(np.concatenate([np.cos(phase), -np.sin(phase)]), 3))

    inner = [(a, z) for a in range(CELL) for z in range(CELL)]
    upper = [(CELL, z) for z in range(CELL)] + [(a, CELL) for a in range(CELL)] + [(CELL, CELL)]
    outer = [(-1, z) for z in range(CELL)] + [(CELL, z) for z in range(CELL)]
    outer += [(a, -1) for a in range(CELL)] + [(a, CELL) for a in range(CELL)]
    used = np.zeros(EDGE)
    used[: len(upper)] = 1.0
    upper = np.array(upper + [(0, 0)] * (EDGE - len(upper)))
    inner, outer = np.array(inner), np.array(outer)

    def inside(cells, sign):
        return np.exp(sign * 2j * np.pi * (cells @ np.array(inner).T) / CELL)

    def twiddles(cells, copies):
        p = np.arange(n)
        phase = 2 * np.pi * (
            np.outer(p // n_pz, cells[:, 0]) / ny + np.outer(p % n_pz, cells[:, 1]) / nz
        )
        return np.tile(np.stack([np.cos(phase), np.sin(phase)]), (1, 1, copies))

    share = lambda at: np.where((at == 0) | (at == CELL), 0.5, 1.0)
    flat = share(inner[:, 0]) * share(inner[:, 1])
    flat_edge = share(upper[:, 0]) * share(upper[:, 1]) * used
    pattern = np.zeros((CELL, 256))
    pattern[0, :CELLS] = flat
    pattern[0, 128 : 128 + EDGE] = flat_edge
    turn = np.concatenate([twiddles(inner, 2), twiddles(upper, 4)], axis=2).reshape(2 * n, 256)
    turn = np.concatenate([turn, pattern]).astype(np.float32)
    unturn = np.concatenate([twiddles(inner, 2), twiddles(outer, 4)], axis=2)
    unturn = unturn.reshape(2 * n, 256).astype(np.float32)

    wave = inside(inner, -1)
    fwd = parts(np.concatenate([real_form(wave, 0), real_form(wave, 1)]), 2)
    fwd = np.concatenate([fwd[0], fwd[1]], axis=1)
    wave = inside(upper, -1) * used[:, None]
    spread = [np.kron(np.eye(2), real_form(wave, t)) for t in range(2)]
    fwd_edge = parts(np.concatenate(spread), 2)
    wave, wave_edge = inside(inner, 1).T, inside(outer, 1).T
    pieces = [real_form(wave, 0), real_form(wave, 1)]
    pieces += [np.tile(real_form(wave_edge, t), (1, 2)) for t in range(2)]
    inv = parts(np.concatenate(pieces, axis=1), 2)
    inv = np.concatenate([inv[0], inv[0], inv[1]])
    return np.stack(line), np.stack(back), fwd, fwd_edge, inv, turn, unturn


def plus(a, b):
    return b if a is None else a if b is None else a + b


def minus(a, b):
    return a if b is None else -b if a is None else a - b


def conj(x):
    return x[0], minus(None, x[1]) if x[1] is not None else None


def add(x, y):
    return plus(x[0], y[0]), plus(x[1], y[1])


def sub(x, y):
    return minus(x[0], y[0]), minus(x[1], y[1])


def rotated(x, k, n, sign):
    re, im = x
    if k == 0:
        return x
    if 4 * k == n:
        turned = (minus(None, im) if im is not None else None, re)
        return turned if sign > 0 else (im, -re)
    c, s = math.cos(2 * math.pi * k / n), sign * math.sin(2 * math.pi * k / n)
    if im is None:
        return re * c, re * s
    if 8 * k == n:
        both = (re - im, re + im) if sign > 0 else (re + im, im - re)
        return both[0] * c, both[1] * c
    return re * c - im * s, re * s + im * c


def fft(x, sign):
    n = len(x)
    if n == 1:
        return x
    even, odd = fft(x[::2], sign), fft(x[1::2], sign)
    odd = [rotated(o, k, n, sign) for k, o in enumerate(odd)]
    return [add(e, o) for e, o in zip(even, odd)] + [sub(e, o) for e, o in zip(even, odd)]


def rfft(x):
    n = len(x)
    if n == 1:
        return [(x[0], None)]
    if n == 2:
        return [(x[0] + x[1], None), (x[0] - x[1], None)]
    even, odd = rfft(x[::2]), rfft(x[1::2])
    out = [None] * (n // 2 + 1)
    for k in range(n // 4 + 1):
        turned = rotated(odd[k], k, n, -1)
        out[k] = add(even[k], turned)
        if k < n // 4:
            out[n // 2 - k] = conj(sub(even[k], turned))
    return out


def irfft(x):
    n = 2 * (len(x) - 1)
    if n == 2:
        return [x[0][0] + x[1][0], x[0][0] - x[1][0]]
    even, odd = [], []
    for k in range(n // 4 + 1):
        if 4 * k == n:
            even.append((x[k][0] * 2.0, None))
            odd.append((x[k][1] * -2.0, None) if x[k][1] is not None else (x[k][0] * 0.0, None))
            continue
        mirror = conj(x[n // 2 - k])
        even.append(add(x[k], mirror))
        odd.append(rotated(sub(x[k], mirror), k, n, 1))
    even, odd = irfft(even), irfft(odd)
    return [v for pair in zip(even, odd) for v in pair]


def plane_forward(values, n_py, n_pz):
    lines = [rfft(row) for row in values]
    out = {}
    for pz in range(n_pz // 2 + 1):
        column = [line[pz] for line in lines]
        if all(x[1] is None for x in column):
            found = rfft([x[0] for x in column])
            found += [conj(found[n_py - py]) for py in range(n_py // 2 + 1, n_py)]
        else:
            found = fft(column, -1)
        for py in range(n_py):
            out[py, pz] = found[py]
    return out


def plane_inverse(half, n_py, n_pz):
    columns = []
    for pz in range(n_pz // 2 + 1):
        if pz in (0, n_pz // 2):
            column = irfft([half[py, pz] for py in range(n_py // 2 + 1)])
            columns.append([(x, None) for x in column])
        else:
            columns.append(fft([half[py, pz] for py in range(n_py)], 1))
    return [irfft([column[ay] for column in columns]) for ay in range(n_py)]


def split(x, count=2):
    out = []
    for i in range(count):
        out.append(x.astype(BF16))
        if i < count - 1:
            x = x - out[-1].astype(F32)
    return out


def dot(left, right, dims=((1,), (0,))):
    return lax.dot_general(left, right, (dims, ((), ())), preferred_element_type=F32)


def dot_parts(left, right, dims=((1,), (0,))):
    count = len(left)
    total = None
    for order in reversed(range(count)):
        for i in range(order + 1):
            term = dot(left[i], right[order - i], dims)
            total = term if total is None else total + term
    return total


def green_factor(owner, parity, n_py, n_pz, nx, nf):
    n = n_py * n_pz
    ny, nz = CELL * n_py, CELL * n_pz
    shape = (n * nf, 128)
    row = lax.broadcasted_iota(jnp.int32, shape, 0)
    col = lax.broadcasted_iota(jnp.int32, shape, 1)

    def square(wave, period):
        folded = jnp.minimum(wave, period - wave).astype(F32)
        return (folded * (2.0 * math.pi / period)) ** 2

    p = row // nf
    wave_x = 2 * (owner * nf + row % nf) + parity
    wave_y = p // n_pz + n_py * (col // CELL % CELL)
    wave_z = p % n_pz + n_pz * (col % CELL)
    total = square(wave_y, ny) + square(wave_z, nz) + square(wave_x, nx)
    safe = jnp.where(total > 0, total, 1.0)
    green = jnp.where(total > 0, -4.0 * math.pi * jnp.exp(-SMOOTHING_SQ * total) / safe, 0.0)
    return green * (jnp.where(wave_x > 0, 1.0, 0.5) * (1.0 / float(ny * nz * nx)))


def kernel(
    n_py, n_pz, nx, nf, chunk,
    pos_hbm, mass_hbm, line_hbm, back_hbm, fwd_hbm, fwd_edge_hbm, inv_hbm, turn_hbm, unturn_hbm,
    pot_ref, side_ref,
    pos_ref, mass_ref, line, back, fwd, fwd_edge, inv, turn, unturn, table_sem,
    piece_sem, acc, green, mixed, send1, recv1, send2, recv2, waves_edge,
    send_sem1, recv_sem1, send_sem2, recv_sem2,
):
    n = n_py * n_pz
    half_nf, half, quarter = nf // 2, nx // 2, nx // 4
    my_y, my_z = lax.axis_index("py"), lax.axis_index("pz")
    rank = my_y * n_pz + my_z

    loads = [
        pltpu.make_async_copy(src, dst, table_sem.at[i])
        for i, (src, dst) in enumerate(
            [
                (line_hbm, line),
                (turn_hbm, turn),
                (fwd_hbm, fwd),
                (fwd_edge_hbm, fwd_edge),
                (inv_hbm, inv),
                (unturn_hbm, unturn),
                (back_hbm, back),
            ]
        )
    ]
    pieces = []
    width = pos_ref.shape[1] // 2
    for i in range(2):
        span = pl.ds(i * width, width)
        for src, dst in ((pos_hbm, pos_ref), (mass_hbm, mass_ref)):
            pieces.append(
                pltpu.make_async_copy(src.at[:, span], dst.at[:, span], piece_sem.at[len(pieces)])
            )
            pieces[-1].start()

    n_own, half_z, first_z = n // 2, n_pz // 2, n_pz // 4
    own_z = my_z - first_z
    is_owner = (own_z >= 0) & (own_z < half_z)
    is_guest = jnp.logical_not(is_owner)
    owner = my_y * half_z + own_z
    turn_z = jnp.where(my_z >= half_z, first_z, 0) ^ lax.rem(my_z, 2)

    def far_first(step):
        along = step % n_pz
        return -(along // 4), -bin(step).count("1"), along % 4 // 2, -step

    everyone, readers, owners = [], [], []
    for step in sorted(range(1, n), key=far_first):
        other_y, other_z = (step // n_pz) ^ my_y, (step % n_pz) ^ my_z
        everyone.append((other_y * n_pz + other_z, (other_y, other_z)))
    core = lax.rem(my_z, 2)
    for step in range(n):
        along = step // (2 * n_py)
        other_y, other_z = step // 2 % n_py, 2 * along + step % 2
        if along:
            other_y, other_z = other_y ^ my_y, other_z ^ core
        readers.append((2 * along, other_y * n_pz + other_z, (other_y, other_z)))
    for step in sorted(range(n_own), key=lambda v: (-(v % half_z // 2), -bin(v // half_z).count("1"))):
        other_y, other_z = (step // half_z) ^ my_y, (step % half_z) ^ turn_z
        place = (other_y, other_z + first_z)
        owners.append((step < half_z, other_y * half_z + other_z, place))

    barrier = pltpu.get_barrier_semaphore()

    @pl.when(is_owner)
    def _():
        for _, where in everyone:
            pl.semaphore_signal(barrier, inc=1, device_id=where, device_id_type=MESH)

    for load in loads:
        load.start()
    base_y = (my_y * CELL).astype(F32)
    base_z = (my_z * CELL).astype(F32)
    row_of = lax.broadcasted_iota(jnp.int32, (CELL, chunk), 0)
    cell = row_of.astype(F32)
    sublane = lax.broadcasted_iota(jnp.int32, (2 * CELL, chunk), 0).astype(F32)

    for load in pieces:
        load.wait()

    def deposited(turn_index):
        span = pl.ds(pl.multiple_of(turn_index * chunk, chunk), chunk)
        tall = (CELL, chunk)
        along_y = jnp.broadcast_to(pos_ref[0:1, span], tall) - base_y
        along_z = jnp.broadcast_to(pos_ref[1:2, span], tall) - base_z
        along_x = jnp.broadcast_to(pos_ref[2:3, span], tall)
        mass = jnp.broadcast_to(mass_ref[0:1, span], tall)
        floor_x = jnp.floor(along_x)
        pair = jnp.floor(along_x * 0.5)
        is_even = floor_x == 2.0 * pair
        upper = mass * (along_x - floor_x)
        lower = mass * (1.0 - (along_x - floor_x))
        shares = [
            jnp.where(is_even, lower, 0.0),
            jnp.where(is_even, upper, lower),
            jnp.where(is_even, 0.0, upper),
        ]
        where_x = jnp.concatenate([pair, pair], axis=0).astype(BF16)
        one_hot = jnp.concatenate(
            [
                jnp.where(
                    where_x == (sublane + float(t)).astype(BF16),
                    jnp.ones((), BF16),
                    jnp.zeros((), BF16),
                )
                for t in range(0, half, 2 * CELL)
            ],
            axis=0,
        )
        hat_y = jnp.maximum(1.0 - jnp.abs(along_y - cell), 0.0)
        hat_z = jnp.maximum(1.0 - jnp.abs(along_z - cell), 0.0)
        last_y = jnp.maximum(along_y - (CELL - 1.0), 0.0)
        last_z = jnp.maximum(along_z - (CELL - 1.0), 0.0)
        tiles = []
        for share in shares:
            scaled = hat_z * share
            tiles += [hat_y[a : a + 1] * scaled for a in range(CELL)]
            tiles += [last_y * scaled, hat_y * (last_z * share)]
        corner = jnp.where(row_of == 0, shares[0], jnp.where(row_of == 1, shares[1], shares[2]))
        tiles.append(jnp.where(row_of < 3, corner * (last_y * last_z), 0.0))
        tiles.append(jnp.zeros(tall, F32))
        return split(jnp.concatenate(tiles, axis=0)), one_hot

    turns = pos_ref.shape[1] // chunk

    acc[...] = jnp.zeros_like(acc)

    @pl.loop(0, turns // 2)
    def _(index):
        for i in range(2):
            masses, one_hot = deposited(2 * index + i)
            acc[i] += dot(jnp.concatenate(masses, axis=0), one_hot, ((1,), (1,)))

    for load in loads[:1]:
        load.wait()
    sums = acc[0] + acc[1]
    sums = sums[: sums.shape[0] // 2] + sums[sums.shape[0] // 2 :]
    block = CELLS + 2 * CELL
    even = sums[:block] + pltpu.roll(sums[2 * block : 3 * block], 1, 1)
    odd = sums[block : 2 * block]
    corner = sums[3 * block : 3 * block + CELL]
    first = lax.broadcasted_iota(jnp.int32, (CELL, half), 0) == 0
    blank = jnp.zeros((CELL, half), F32)
    corner_even = corner + pltpu.roll(pltpu.roll(corner, CELL - 2, 0), 1, 1)
    corner_even = jnp.where(first, corner_even, 0.0)
    corner_odd = jnp.where(first, pltpu.roll(corner, CELL - 1, 0), 0.0)
    even = jnp.concatenate([even, corner_even, blank], axis=0)
    odd = jnp.concatenate([odd, corner_odd, blank], axis=0)

    lane = lax.broadcasted_iota(jnp.int32, (nf, 128), 1)
    is_real = lane < CELLS
    is_real_edge = lane % CELLS < EDGE
    low_half = lax.broadcasted_iota(jnp.int32, (half_nf, 128), 1) < CELLS
    for parity in range(2):
        folded = []
        for grid in (even, odd):
            left, right = grid[:, :quarter], grid[:, quarter:]
            folded.append(left - right if parity else left + right)
        density = [
            jnp.concatenate([x[:CELLS]] * 2 + [x[CELLS:]] * 4, axis=0)
            for x in split(jnp.concatenate(folded, axis=1))
        ]
        both = dot_parts([line[parity, 0], line[parity, 1]], density, ((1,), (1,)))
        for r in range(n_own):
            re, im = both[r * nf : (r + 1) * nf], both[quarter + r * nf : quarter + (r + 1) * nf]
            send1[parity, r, 0:nf] = jnp.where(is_real, re[:, :128], im[:, :128])
            side = jnp.where(is_real_edge, re[:, 128:], im[:, 128:])
            send1[parity, r, nf : nf + half_nf] = jnp.where(
                low_half, side[:half_nf], side[half_nf:]
            )
        if parity == 0:

            @pl.when(is_owner)
            def _():
                pl.semaphore_wait(barrier, n_own - 1)

            @pl.when(is_guest)
            def _():
                pl.semaphore_wait(barrier, n_own)

        for maybe_self, peer, where in owners:
            copy = pltpu.make_async_remote_copy(
                src_ref=send1.at[parity, peer],
                dst_ref=recv1.at[parity, rank],
                send_sem=send_sem1.at[parity],
                recv_sem=recv_sem1.at[parity],
                device_id=where,
                device_id_type=MESH,
            )
            if maybe_self:
                pl.when(where[1] != my_z)(copy.start)
            else:
                copy.start()

    def wait_for(ref, parity, count, sem):
        span = ref.at[parity, pl.ds(0, count)]
        pltpu.make_async_copy(span, span, sem.at[parity]).wait()

    def every(half_plane, py, pz):
        if pz <= n_pz // 2:
            return half_plane[py, pz], 1
        return half_plane[-py % n_py, n_pz - pz], -1

    def middle(parity):
        turned = []
        for lanes, span, height in (
            (slice(0, 128), slice(0, nf), nf),
            (slice(128, 256), slice(nf, nf + half_nf), half_nf),
        ):
            values = [[recv1[parity, ay * n_pz + az, span] for az in range(n_pz)] for ay in range(n_py)]
            found = plane_forward(values, n_py, n_pz)
            blocks = []
            for p in range(n):
                (re, im), sign = every(found, p // n_pz, p % n_pz)
                c, s = turn[p : p + 1, lanes], turn[n + p : n + p + 1, lanes]
                if im is None:
                    u, v = c * re, -(s * re)
                elif sign > 0:
                    u, v = c * re + s * im, c * im - s * re
                else:
                    u, v = c * re - s * im, -(c * im) - s * re
                blocks.append([u, v])
            turned.append(blocks)
        if parity == 0:
            corner_row = lax.broadcasted_iota(jnp.int32, (half_nf, 128), 0) == 0
            top_row = lax.broadcasted_iota(jnp.int32, (nf, 128), 0) == 0
            level = jnp.sum(turned[0][0][0][0:1] * jnp.where(is_real[0:1], 1.0, 0.0), axis=1, keepdims=True)
            level += jnp.sum(
                turned[1][0][0][0:1] * jnp.where(lane[0:1] < EDGE, 1.0, 0.0), axis=1, keepdims=True
            )
            level = jnp.where(owner == 0, level * (1.0 / CELLS), 0.0)
            flat = turn[2 * n : 2 * n + 1]
            turned[0][0][0] = turned[0][0][0] - jnp.where(top_row, level * flat[:, :128], 0.0)
            turned[1][0][0] = turned[1][0][0] - jnp.where(corner_row, level * flat[:, 128:], 0.0)

        stacked = [
            jnp.concatenate(
                [jnp.concatenate([uv[i] for uv in blocks], axis=0) for i in range(2)], axis=1
            )
            for blocks in turned
        ]
        count = n * nf
        wide = dot(jnp.concatenate(split(stacked[0]), axis=0), fwd[...])
        solved = wide[:count, :128] + wide[:count, 128:] + wide[count:, :128]
        beside = dot_parts(split(stacked[1]), [fwd_edge[0], fwd_edge[1]])
        pieces = []
        for p in range(n):
            rows_of = beside[p * half_nf : (p + 1) * half_nf]
            pieces += [rows_of[:, :128], rows_of[:, 128:]]
        solved = (solved + jnp.concatenate(pieces, axis=0)) * green[parity]
        high, low = split(solved)
        mixed[...] = dot(jnp.concatenate([high, low], axis=1), inv[0:256]) + dot(high, inv[256:384])

        for lanes, offset in ((slice(0, 128), 0), (slice(128, 256), 256)):
            ones, twos = {}, {}
            for p in range(n):
                c, s = unturn[p : p + 1, lanes], unturn[n + p : n + p + 1, lanes]
                span = slice(p * nf, (p + 1) * nf)
                y, jy = mixed[span, offset : offset + 128], mixed[span, offset + 128 : offset + 256]
                ones[p // n_pz, p % n_pz] = c * y + s * jy
                twos[p // n_pz, p % n_pz] = c * jy - s * y
            half_plane = {}
            for pz in range(n_pz // 2 + 1):
                for py in range(n_py):
                    other = (-py % n_py, -pz % n_pz)
                    if other == (py, pz):
                        half_plane[py, pz] = (ones[other] * 2.0, None)
                    else:
                        half_plane[py, pz] = (
                            ones[py, pz] + ones[other],
                            twos[other] - twos[py, pz],
                        )
            values = plane_inverse(half_plane, n_py, n_pz)
            for ay in range(n_py):
                for az in range(n_pz):
                    value = values[ay][az]
                    if offset == 0:
                        send2[parity, ay * n_pz + az, 0:nf] = value
                    else:
                        value = jnp.where(low_half, value[:half_nf], value[half_nf:])
                        send2[parity, ay * n_pz + az, nf : nf + half_nf] = value
        def deliver(which, chosen):
            for along, peer, where in readers:
                if along not in chosen:
                    continue
                copy = pltpu.make_async_remote_copy(
                    src_ref=send2.at[which, peer],
                    dst_ref=recv2.at[which, owner],
                    send_sem=send_sem2.at[which],
                    recv_sem=recv_sem2.at[which],
                    device_id=where,
                    device_id_type=MESH,
                )
                if first_z <= along < first_z + half_z:
                    pl.when(peer != rank)(copy.start)
                else:
                    copy.start()

        planes = list(range(0, n_pz, 2))
        near, far = planes[:1], planes[-1:]
        inner = planes[1:-1]
        half_in = len(inner) // 2
        if parity == 0:
            deliver(0, near + far)
        else:
            deliver(1, near + far)
            for along in inner:
                deliver(0, [along])
                deliver(1, [along])
        recv2[parity, owner] = send2[parity, rank]

    @pl.when(is_owner)
    def _():
        for parity in range(2):
            recv1[parity, rank] = send1[parity, owner]
            green[parity] = green_factor(owner, parity, n_py, n_pz, nx, nf)
        for load in loads[1:6]:
            load.wait()
        for parity in range(2):
            with jax.named_scope("wait1"):
                wait_for(recv1, parity, n - 1, recv_sem1)
            with jax.named_scope("mid"):
                middle(parity)

    @pl.when(is_guest)
    def _():
        for load in loads[1:6]:
            load.wait()

    loads[6].wait()
    found = []
    for parity in range(2):
        with jax.named_scope("wait2"):

            @pl.when(is_owner)
            def _():
                wait_for(recv2, parity, n_own - 1, recv_sem2)

            @pl.when(is_guest)
            def _():
                wait_for(recv2, parity, n_own, recv_sem2)

        for r in range(n_own):
            waves_edge[r * half_nf : (r + 1) * half_nf] = recv2[parity, r, nf : nf + half_nf]
        beside = jnp.transpose(waves_edge[...])
        rows_of = [
            recv2[parity, r, h * half_nf : (h + 1) * half_nf]
            for h in range(2)
            for r in range(n_own)
        ]
        inner = jnp.transpose(jnp.concatenate(rows_of, axis=0))
        columns = []
        for c in range(2):
            pieces = [
                beside[h * CELLS + c * EDGE : h * CELLS + (c + 1) * EDGE] for h in range(2)
            ]
            columns.append(
                jnp.concatenate(
                    [inner[c * CELLS : (c + 1) * CELLS], jnp.concatenate(pieces, axis=1)], axis=0
                )
            )
        found.append(
            dot_parts(
                split(jnp.concatenate(columns, axis=1), 3), [back[parity, i] for i in range(3)]
            )
        )
    for side, value in enumerate((found[0] + found[1], found[0] - found[1])):
        span = slice(side * half, (side + 1) * half)
        for a in range(CELL):
            pot_ref[a, :, span] = value[a * CELL : (a + 1) * CELL]
        for i in range(4):
            side_ref[i, :, span] = value[CELLS + i * CELL : CELLS + (i + 1) * CELL]

    @pl.when(is_owner)
    def _():
        for parity in range(2):
            wait_for(send1, parity, n_own - 1, send_sem1)
            wait_for(send2, parity, n - 1, send_sem2)

    @pl.when(is_guest)
    def _():
        for parity in range(2):
            wait_for(send1, parity, n_own, send_sem1)


def finish(pot_ref, side_ref, out_hbm, out_ref, sems):
    nx = pot_ref.shape[2]
    copies = []

    def emit(d):
        copies.append(pltpu.make_async_copy(out_ref.at[d], out_hbm.at[d], sems.at[d]))
        copies[-1].start()

    for a in range(CELL):
        tile = pot_ref[a]
        out_ref[2, a] = (pltpu.roll(tile, 1, 1) - pltpu.roll(tile, nx - 1, 1)) * 0.5
    emit(2)
    for a in range(CELL):
        below = pot_ref[a - 1] if a else side_ref[0]
        above = pot_ref[a + 1] if a < CELL - 1 else side_ref[1]
        out_ref[0, a] = (below - above) * 0.5
    emit(0)
    before, after = side_ref[2], side_ref[3]
    lane_row = lax.broadcasted_iota(jnp.int32, (CELL, nx), 0)
    for a in range(CELL):
        tile = pot_ref[a]
        lower = jnp.where(lane_row == 0, before[a : a + 1], pltpu.roll(tile, 1, 0))
        upper = jnp.where(lane_row == CELL - 1, after[a : a + 1], pltpu.roll(tile, CELL - 1, 0))
        out_ref[1, a] = (lower - upper) * 0.5
    emit(1)
    for copy in copies:
        copy.wait()


def solution(mesh):
    n_py, n_pz = mesh.shape["py"], mesh.shape["pz"]
    n = n_py * n_pz
    nx = 512
    nf = nx // 4 // (n // 2)
    consts = tables(n_py, n_pz, nx, nf)

    def shards(positions, masses):
        chunk = positions.shape[1] // 2
        vmem = pl.BlockSpec(memory_space=pltpu.VMEM)
        hbm = pl.BlockSpec(memory_space=pltpu.HBM)
        dma = pltpu.SemaphoreType.DMA
        rows = nf + nf // 2
        few, all_of = (pltpu.VMEM((2, count, rows, 128), F32) for count in (n // 2, n))
        operands = [positions, masses.reshape(1, -1), *map(jnp.asarray, consts)]
        pot, side = pl.pallas_call(
            functools.partial(kernel, n_py, n_pz, nx, nf, chunk),
            out_shape=[pltpu.VMEM((CELL, CELL, nx), F32), pltpu.VMEM((4, CELL, nx), F32)],
            in_specs=[hbm] * len(operands),
            out_specs=[vmem, vmem],
            scratch_shapes=[
                *[pltpu.VMEM(x.shape, x.dtype) for x in operands],
                dma((len(operands),)),
                dma((4,)),
                pltpu.VMEM((2, 2 * (3 * (CELLS + 2 * CELL) + 2 * CELL), nx // 2), F32),
                pltpu.VMEM((2, n * nf, 128), F32),
                pltpu.VMEM((n * nf, 512), F32),
                few, all_of, all_of, few,
                pltpu.VMEM((n // 2 * (nf // 2), 128), F32),
                dma((2,)), dma((2,)), dma((2,)), dma((2,)),
            ],
            compiler_params=pltpu.CompilerParams(
                collective_id=0, has_side_effects=True, vmem_limit_bytes=50 << 20
            ),
        )(*[pltpu.with_memory_space_constraint(x, pltpu.HBM) for x in operands])
        return pl.pallas_call(
            finish,
            out_shape=jax.ShapeDtypeStruct((3, CELL, CELL, nx), F32),
            in_specs=[vmem, vmem],
            out_specs=hbm,
            scratch_shapes=[pltpu.VMEM((3, CELL, CELL, nx), F32), dma((3,))],
            compiler_params=pltpu.CompilerParams(vmem_limit_bytes=16 << 20),
        )(pot, side)

    return jax.shard_map(
        shards,
        mesh=mesh,
        in_specs=(P(None, ("py", "pz")), P(("py", "pz"))),
        out_specs=P(None, "py", "pz", None),
        check_vma=False,
    )
```
